32 devices in a mesh: dom: 4 (over x, core), orb: 8 (over z, y).
Axes of the slice: x: 2, y: 2, z: 4, core: 2. Of those that a mesh axis runs over, the one named last changes fastest.
Arguments:
- orbitals: float32 [4, 16, 48, 2304], P('dom', 'orb'), may hold values from -6 to 6
- occupations: float32 [4, 16], P('dom', 'orb'), may hold values from 0.25 to 2
- occupied_count: int32 [4], P('dom'), may hold values from 4 to 16
- weights: float32 [4, 48], P('dom'), may hold values from 0 to 1, as said below
- external_potential: float32 [4, 48, 2304], P('dom'), may hold values from -2 to 0.5
- core_density: float32 [4, 48, 2304], P('dom'), may hold values from 0.08 to 2.88, as said below
- hartree_guess: float32 [128, 2304], P(('dom', 'orb')), may hold values from -6 to 6
Outputs:
- potential: float32 [128, 2304], P(('dom', 'orb'))
The draws below stay inside these ranges and needn't reach their ends.
Inputs may be any that keep to these rules, and one draw needn't show every extreme that they name: orbitals 0 to occupied_count - 1 of a domain are occupied. `weights`: positive; on every global plane the weights of the boxes that cover it sum to one. `core_density`: positive.
All inputs are finite; a program needn't handle non-finite values.
Results may differ from the reference program's by a relative error of at most 0.00017.
Values sent between devices are 32-bit elements; how exact they have to be, the bound alone decides.
A program may use at most 64 MiB of HBM per device.

```python
import math
import jax
import jax.numpy as jnp
from jax import lax

SIDE = 48
CORE = 32
BUF = 8
DEGREE = 8
SWEEPS = 4
CYCLES = 2
DOMAINS = 4
ORBS = 16
BOX = 48
GX = 128


def draw_weights(key, part):
    samples = jnp.exp(jax.random.uniform(key, (DOMAINS, BOX), jnp.float32, -1.6094, 1.6094))
    position = (jnp.arange(DOMAINS, dtype=jnp.int32)[:, None] * CORE - BUF + jnp.arange(BOX, dtype=jnp.int32)[None, :]) % GX
    totals = jnp.zeros((GX,), jnp.float32).at[position.reshape(-1)].add(samples.reshape(-1))
    return samples / totals[position]


def draw_core_density(key, part):
    ladder = jnp.arange(DOMAINS, dtype=jnp.float32) / max(DOMAINS - 1, 1)
    scales = 0.3 * 3.0 ** ladder
    roughness = jax.random.uniform(key, (DOMAINS, BOX, SIDE * SIDE), jnp.float32, 0.4, 1.6)
    return scales[:, None, None] * roughness


def set_ends(drawn, key, smallest, high):
    dims = drawn.shape
    spot = [jax.random.randint(jax.random.fold_in(key, axis), (), 0, dims[axis]) for axis in range(len(dims))]
    drawn = drawn.at[tuple(spot)].set(smallest)
    longest = dims.index(max(dims))
    spot[longest] = (spot[longest] + 1) % dims[longest]
    return drawn.at[tuple(spot)].set(high)


def level_of(rng, shape, pieces, low, high):
    def one(axis_at, blocks):
        draws = jax.random.uniform(jax.random.fold_in(jax.random.fold_in(rng, 6), axis_at), (blocks,), jnp.float32, low / len(pieces), high / len(pieces))
        return jnp.repeat(jnp.exp(draws), shape[axis_at] // blocks).reshape((-1,) + (1,) * (len(shape) - axis_at - 1))

    factor_of = one(*pieces[0])
    for cut in pieces[1:]:
        factor_of = factor_of * one(*cut)
    return factor_of


def bell_draw(stream_key, extent, scale, most, shards=(), kind=jnp.bfloat16):
    gain = level_of(stream_key, extent, shards, -0.22, 0.18) if shards else 1.0
    array = jax.random.normal(stream_key, extent, jnp.float32) * scale * gain
    return jnp.minimum(jnp.maximum(array, -most), most).astype(kind)


def setup_inputs(seed: int = 0) -> dict:
    key_list = jax.random.split(jax.random.key(seed), 8)
    return {
        "orbitals": bell_draw(key_list[0], (DOMAINS, ORBS, BOX, SIDE * SIDE), 1.0, 6.0, ((0, 4), (1, 8)), jnp.float32),
        "occupations": jnp.clip(jnp.exp(math.log(2.0) - 2.0794415 * jax.random.uniform(key_list[1], (DOMAINS, ORBS), jnp.float32) ** level_of(key_list[1], (DOMAINS, ORBS), ((0, 4), (1, 8)), -0.2, 0.2)), 0.25, 2.0),
        "occupied_count": set_ends(jax.random.randint(key_list[2], (DOMAINS,), ORBS // 4, ORBS + 1), jax.random.fold_in(key_list[2], 1), ORBS // 4, ORBS).astype(jnp.int32),
        "weights": draw_weights(jax.random.fold_in(key_list[7], 71), 0),
        "external_potential": jnp.clip(-2.0 + 2.5 * jax.random.uniform(key_list[4], (DOMAINS, BOX, SIDE * SIDE), jnp.float32) ** level_of(key_list[4], (DOMAINS, BOX, SIDE * SIDE), ((0, 4),), -0.2, 0.2), -2.0, 0.5),
        "core_density": draw_core_density(jax.random.fold_in(key_list[7], 71), 0),
        "hartree_guess": bell_draw(key_list[6], (GX, SIDE * SIDE), 1.0, 6.0, ((0, 32),), jnp.float32),
    }


EXCHANGE_FACTOR = (3.0 / 3.141592653589793) ** (1.0 / 3.0)
FOUR_PI = 4.0 * 3.141592653589793
RELAXATION = 0.8
CUTOFF = 1.5

def transverse_sum(field):
    cells = field.shape[-1]
    column = jnp.arange(cells, dtype=jnp.int32) % SIDE
    left = jnp.where(column == 0, jnp.roll(field, -(SIDE - 1), -1), jnp.roll(field, 1, -1))
    right = jnp.where(column == SIDE - 1, jnp.roll(field, SIDE - 1, -1), jnp.roll(field, -1, -1))
    return left + right + jnp.roll(field, SIDE, -1) + jnp.roll(field, -SIDE, -1)

def hamiltonian(orbital_set, box_potential):
    padded = jnp.pad(orbital_set, ((0, 0), (1, 1), (0, 0)))
    neighbours = padded[:, 2:] + padded[:, :-2] + transverse_sum(orbital_set)
    return 0.5 * (6.0 * orbital_set - neighbours) + box_potential[None] * orbital_set

def chebyshev(orbital_set, box_potential):
    low_bound = jnp.min(box_potential) + CUTOFF
    high_bound = jnp.max(box_potential) + 6.0
    center = 0.5 * (high_bound + low_bound)
    half_width = 0.5 * (high_bound - low_bound)
    previous = orbital_set
    current = (hamiltonian(orbital_set, box_potential) - center * orbital_set) / half_width
    for step_index in range(DEGREE - 1):
        following = 2.0 * (hamiltonian(current, box_potential) - center * current) / half_width - previous
        previous, current = (current, following)
    return current

def reference(orbitals, occupations, occupied_count, weights, external_potential, core_density, hartree_guess):
    box_starts = jnp.arange(DOMAINS, dtype=jnp.int32) * CORE - BUF
    plane_index = (box_starts[:, None] + jnp.arange(BOX, dtype=jnp.int32)[None, :]) % GX
    occupied = jnp.arange(ORBS, dtype=jnp.int32)[None, :] < occupied_count[:, None]
    factors = jnp.where(occupied, occupations, jnp.float32(0.0)) / ORBS
    orbital_set = orbitals
    hartree = hartree_guess
    scf_box = jnp.zeros_like(external_potential)
    potential = hartree_guess
    for cycle_index in range(CYCLES):
        box_potential = external_potential + scf_box

        def one_domain(domain_item):
            domain_orbitals, domain_potential, factor_row = domain_item
            filtered = chebyshev(domain_orbitals, domain_potential)
            squares = lax.optimization_barrier(jnp.mean(filtered * filtered, axis=(1, 2))) + 1e-06
            filtered = filtered / jnp.sqrt(squares)[:, None, None]
            density_part = lax.optimization_barrier(jnp.sum(factor_row[:, None, None] * filtered * filtered, axis=0))
            return (filtered, density_part)
        orbital_set, density_part = lax.map(one_domain, (orbital_set, box_potential, factors))
        weighted = (density_part + core_density) * weights[:, :, None]
        density = jnp.zeros((GX, SIDE * SIDE), jnp.float32).at[plane_index.reshape(-1)].add(weighted.reshape(-1, SIDE * SIDE))
        average = jnp.mean(density)
        source = FOUR_PI * (density - average)
        for sweep_index in range(SWEEPS):
            neighbours = jnp.roll(hartree, 1, 0) + jnp.roll(hartree, -1, 0) + transverse_sum(hartree)
            hartree = hartree + RELAXATION * ((neighbours + source) / 6.0 - hartree)
        potential = hartree - EXCHANGE_FACTOR * jnp.cbrt(density)
        scf_box = potential[plane_index]
    return potential
```

```python
import functools

import jax
import jax.numpy as jnp
from jax import lax
from jax.experimental import pallas as pl
from jax.experimental.pallas import tpu as pltpu
from jax.sharding import PartitionSpec as P

SIDE = 48
BUF = 8
DEGREE = 8
SWEEPS = 4
CYCLES = 2
LANES = 128
HALF = 64
SEGMENTS = 4
GROUP = 4


EXCHANGE_FACTOR = (3.0 / 3.141592653589793) ** (1.0 / 3.0)
FOUR_PI = 4.0 * 3.141592653589793
RELAXATION = 0.8
CUTOFF = 1.5


MESH = pl.DeviceIdType.MESH


class Segments:
    def __init__(self, count, box, cells):
        self.count, self.box, self.cells = count, box, cells
        self.lines = cells // SIDE // SEGMENTS
        self.across = LANES // (SEGMENTS * count)
        self.deep = box // self.across
        self.length = self.lines * SIDE
        self.tiles = cells // LANES
        self.blocks = -(-self.length // LANES)
        self.shift = count * self.across
        assert self.deep * self.across == box and self.length % HALF == 0
        assert self.tiles * LANES == cells and SIDE % 8 == 0 and box % 8 == 0

    def spread(self, load, store):
        lane = lax.broadcasted_iota(jnp.int32, (self.across, LANES), 1)
        for plane in range(self.deep):
            kept = {}

            def tile_of(orbital, tile, turned):
                if (orbital, tile, turned) not in kept:
                    value = load(orbital, tile, plane)
                    kept[orbital, tile, turned] = pltpu.roll(value, HALF, 1) if turned else value
                return kept[orbital, tile, turned]

            for block in range(self.blocks):
                rows = min(LANES, self.length - block * LANES)
                pieces = []
                for segment in range(SEGMENTS):
                    first = segment * self.length + block * LANES
                    for orbital in range(self.count):
                        parts = []
                        for half in range(2):
                            cell = min(first + half * HALF, self.cells - HALF)
                            turned = cell % LANES != half * HALF
                            parts.append(tile_of(orbital, cell // LANES, turned))
                        if rows <= HALF or parts[0] is parts[1]:
                            pieces.append(parts[0])
                        else:
                            pieces.append(jnp.where(lane < HALF, parts[0], parts[1]))
                turned = jnp.concatenate(pieces, axis=0).T
                for row in range(0, rows, 8):
                    store(plane, block * LANES + row, turned[row : row + 8])

    def gather(self, load, store):
        lane = lax.broadcasted_iota(jnp.int32, (self.across, LANES), 1)
        for plane in range(self.deep):
            sums = {}
            for block in range(self.blocks):
                rows = min(LANES, self.length - block * LANES)
                pieces = [load(plane, block * LANES + row) for row in range(0, rows, 8)]
                if rows < LANES:
                    pieces.append(jnp.zeros((LANES - rows, LANES), jnp.float32))
                turned = jnp.concatenate(pieces, axis=0).T
                for segment in range(SEGMENTS):
                    base = segment * self.shift
                    value = turned[base : base + self.across]
                    for orbital in range(1, self.count):
                        at = base + orbital * self.across
                        value = value + turned[at : at + self.across]
                    sums[segment, block, False] = value

            def half_of(cell, half):
                segment, place = cell // self.length, cell % self.length
                turned = place % LANES != half * HALF
                key = (segment, place // LANES, turned)
                if key not in sums:
                    sums[key] = pltpu.roll(sums[key[0], key[1], False], HALF, 1)
                return sums[key]

            for tile in range(self.tiles):
                low = half_of(tile * LANES, 0)
                high = half_of(tile * LANES + HALF, 1)
                store(plane, tile, low if low is high else jnp.where(lane < HALF, low, high))


def filter_step(shape, source, target, scale, inverse, first):
    lines, deep, across = shape.lines, shape.deep, shape.across
    lane = lax.broadcasted_iota(jnp.int32, (1, 8, LANES), 2) % across
    has_left = jnp.broadcast_to(lane != 0, (GROUP, 8, LANES))
    has_right = jnp.broadcast_to(lane != across - 1, (GROUP, 8, LANES))

    def turn(value, amount):
        return pltpu.roll(value.reshape(-1, LANES), amount, 1).reshape(value.shape)

    for base in range(0, SIDE, 8):
        cells = slice(8 + base, 16 + base)

        def line(plane, at):
            return source[plane * lines + at : plane * lines + at + 1, cells, :]

        for start in range(0, lines, GROUP):
            middles = [
                source[plane * lines + start : plane * lines + start + GROUP, cells, :]
                for plane in range(deep)
            ]
            for plane in range(deep):
                block = slice(plane * lines + start, plane * lines + start + GROUP)
                middle = middles[plane]
                if plane > 0:
                    left = middles[plane - 1]
                else:
                    left = jnp.where(has_left, turn(middles[deep - 1], 1), 0.0)
                if plane < deep - 1:
                    right = middles[plane + 1]
                else:
                    right = jnp.where(has_right, turn(middles[0], LANES - 1), 0.0)
                if start > 0:
                    below = line(plane, start - 1)
                else:
                    below = turn(line(plane, lines - 1), shape.shift)
                if start + GROUP < lines:
                    above = line(plane, start + GROUP)
                else:
                    above = turn(line(plane, 0), LANES - shape.shift)
                below = jnp.concatenate([below, middle[:-1]], axis=0)
                above = jnp.concatenate([middle[1:], above], axis=0)
                near = source[block, 7 + base : 15 + base, :] + source[block, 9 + base : 17 + base, :]
                near = near + (below + above)
                near = near + (left + right)
                value = scale[block, base : base + 8, :] * middle - inverse * near
                if first:
                    value = 0.5 * value
                else:
                    value = value - target[block, cells, :]
                target[block, cells, :] = value
                if base == 0:
                    target[block, 8 + SIDE : 9 + SIDE, :] = value[:, :1, :]
                if base == SIDE - 8:
                    target[block, 7:8, :] = value[:, 7:, :]


def cycles_kernel(doms, ranks, *refs):
    (
        orbitals_hbm, occupations, counts, weights, ionic_hbm, core_hbm, hartree_hbm,
        output,
        planes_of, ionic, core, flat, weight_rows, even, odd, scale, charge,
        weighted, rim_in, parts, near_h, near_d, work, work_d, box_pot, sums, dom_sums,
        load_sem, rim_send, rim_recv, part_send, part_recv, h_send, h_recv, d_send, d_recv,
        sum_send, sum_recv, dom_send, dom_recv, box_send, box_recv, relay_send,
    ) = refs
    count, box, cells = orbitals_hbm.shape
    chunks, planes, _ = weighted.shape
    shape = Segments(count, box, cells)
    tiles = shape.tiles
    rim = BUF // planes
    reach = near_h.shape[1] // 2
    everyone = doms * ranks
    dom = lax.axis_index("dom")
    rank = lax.axis_index("orb")
    me = dom * ranks + rank

    def place(index):
        return (lax.div(index, ranks), lax.rem(index, ranks))

    def send(source, target, send_sem, recv_sem, to):
        return pltpu.make_async_remote_copy(
            src_ref=source, dst_ref=target, send_sem=send_sem, recv_sem=recv_sem,
            device_id=to, device_id_type=MESH,
        )

    def repeat(low, high, step):
        lax.fori_loop(low, high, lambda i, carry: (step(i), carry)[1], 0)

    def arrived(target, sem):
        send(target, target, sem, sem, (dom, rank)).wait_recv()

    def loads(source, target, sem):
        for tile in range(tiles):
            pltpu.make_async_copy(
                source.at[:, tile * LANES : (tile + 1) * LANES],
                target.at[tile],
                sem,
            ).start()

    def loaded(target, sem):
        pltpu.make_async_copy(target, target, sem).wait()

    loads(ionic_hbm, ionic, load_sem.at[0])
    for orbital in range(count):
        loads(orbitals_hbm.at[orbital], planes_of.at[orbital], load_sem.at[1 + orbital])
    guess = pltpu.make_async_copy(hartree_hbm, near_h.at[0, reach], load_sem.at[1 + count])
    guess.start()
    loads(core_hbm, core, load_sem.at[2 + count])

    barrier = pltpu.get_barrier_semaphore()

    def greet(k):
        pl.semaphore_signal(
            barrier, inc=1, device_id=place(lax.rem(me + k, everyone)), device_id_type=MESH
        )

    repeat(1, everyone, greet)

    sublane = lax.broadcasted_iota(jnp.int32, (8, LANES), 0)
    for group in range(0, box, 8):
        rows = jnp.full((8, LANES), weights[0, group], jnp.float32)
        for row in range(1, 8):
            rows = jnp.where(sublane == row, weights[0, group + row], rows)
        weight_rows[group : group + 8, :] = rows

    lane = lax.broadcasted_iota(jnp.int32, (8, LANES), 1)
    orbital_of = lax.rem(lax.div(lane, shape.across), count)

    def strided(ref, tile, plane):
        return ref[tile, pl.ds(plane, shape.across, stride=shape.deep), :]

    def place_of(plane, cell):
        return plane * shape.lines + cell // SIDE, cell % SIDE

    def store_orbitals(plane, cell, value):
        line, at = place_of(plane, cell)
        even[line, 8 + at : 16 + at, :] = value
        if at == 0:
            even[line, 8 + SIDE : 9 + SIDE, :] = value[:1]
        if at == SIDE - 8:
            even[line, 7:8, :] = value[7:]

    def store_scale(plane, cell, value):
        line, at = place_of(plane, cell)
        scale[line, at : at + 8, :] = value

    def near_copies(cycle, buffer, send_sems, recv_sems):
        copies = []
        for k in range(1, reach + 1):
            for sign in (1, -1):
                to = place(lax.rem(me + sign * k + everyone, everyone))
                slot = reach - sign * k
                copies.append(
                    send(
                        buffer.at[cycle, reach], buffer.at[cycle, slot],
                        send_sems.at[cycle, slot], recv_sems.at[cycle, slot], to,
                    )
                )
        return copies

    factors = []
    for orbital in range(count):
        taken = rank * count + orbital < counts[0]
        factors.append(
            jnp.where(taken, occupations[0, orbital], jnp.float32(0.0)) / (ranks * count)
        )
    norms = [jnp.float32(1.0)] * count
    h_copies = None

    for cycle in range(CYCLES):
        last = cycle + 1 == CYCLES
        if cycle == 0:
            loaded(ionic, load_sem.at[0])
            flat[...] = ionic[...]
        else:
            for tile in range(tiles):
                lanes = slice(tile * LANES, (tile + 1) * LANES)
                for group in range(0, box, 8):
                    first = group // planes
                    pieces = [box_pot[first + i, :, lanes] for i in range(8 // planes)]
                    flat[tile, group : group + 8, :] = ionic[
                        tile, group : group + 8, :
                    ] + jnp.concatenate(pieces, axis=0)
        potential = flat[...]
        lowest = jnp.min(jnp.min(potential, axis=0), axis=0, keepdims=True)
        lowest = jnp.min(lowest, axis=1, keepdims=True)
        highest = jnp.max(jnp.max(potential, axis=0), axis=0, keepdims=True)
        highest = jnp.max(highest, axis=1, keepdims=True)
        low_bound = lowest + CUTOFF
        high_bound = highest + 6.0
        center = 0.5 * (high_bound + low_bound)
        inverse = 1.0 / (0.5 * (high_bound - low_bound))
        flat[...] = (2.0 * inverse) * ((3.0 - center) + potential)
        shape.spread(lambda _, tile, plane: strided(flat, tile, plane), store_scale)
        if cycle == 0:
            for orbital in range(count):
                loaded(planes_of.at[orbital], load_sem.at[1 + orbital])
            shape.spread(
                lambda orbital, tile, plane: strided(planes_of.at[orbital], tile, plane),
                store_orbitals,
            )

        filter_step(shape, even, odd, scale, inverse, True)
        if cycle == 0:
            pl.semaphore_wait(barrier, everyone - 1)
            guess.wait()
            h_copies = near_copies(0, near_h, h_send, h_recv)
            for copy in h_copies:
                copy.start()

        def two_steps(step, carry):
            filter_step(shape, odd, even, scale, inverse, False)
            filter_step(shape, even, odd, scale, inverse, False)
            return carry

        lax.fori_loop(0, (DEGREE - 1) // 2, two_steps, 0)
        filter_step(shape, odd, even, scale, inverse, False)

        total = jnp.zeros((8, LANES), jnp.float32)
        for base in range(0, SIDE, 8):
            value = even[: shape.deep * shape.lines, 8 + base : 16 + base, :]
            total = total + jnp.sum(value * value, axis=0)
        shares = jnp.zeros((8, LANES), jnp.float32)
        for orbital in range(count):
            square = jnp.sum(
                jnp.where(orbital_of == orbital, total, 0.0), axis=0, keepdims=True
            )
            square = jnp.sum(square, axis=1, keepdims=True)
            square = norms[orbital] * square * (1.0 / (box * cells)) + 1e-06
            share = factors[orbital] * norms[orbital] / square
            shares = jnp.where(orbital_of == orbital, share, shares)
            norms[orbital] = norms[orbital] / square

        def load_density(plane, cell):
            line, at = place_of(plane, cell)
            value = even[line, 8 + at : 16 + at, :]
            return shares * (value * value)

        def store_density(plane, tile, value):
            flat[tile, pl.ds(plane, shape.across, stride=shape.deep), :] = value

        shape.gather(load_density, store_density)
        if cycle == 0:
            loaded(core, load_sem.at[2 + count])
        found = jnp.zeros((8, LANES), jnp.float32) if cycle == 0 else charge[...]
        for group in range(0, box, 8):
            rows = slice(group, group + 8)
            weight = weight_rows[rows, :]
            for tile in range(tiles):
                density = flat[tile, rows, :] + core[tile, rows, :] * (1.0 / ranks)
                density = density * weight
                found = found + density
                for piece in range(8 // planes):
                    weighted[
                        group // planes + piece, :, tile * LANES : (tile + 1) * LANES
                    ] = density[piece * planes : (piece + 1) * planes]
        charge[...] = found

        down = (lax.rem(dom + doms - 1, doms), rank)
        up = (lax.rem(dom + 1, doms), rank)
        rims = [
            send(
                weighted.at[:rim], rim_in.at[cycle, 1],
                rim_send.at[cycle, 1], rim_recv.at[cycle, 1], down,
            ),
            send(
                weighted.at[rim + ranks :], rim_in.at[cycle, 0],
                rim_send.at[cycle, 0], rim_recv.at[cycle, 0], up,
            ),
        ]
        for copy in rims:
            copy.start()

        def sum_copy(k):
            to = (dom, lax.rem(rank + k, ranks))
            return send(sums.at[rank], sums.at[rank], sum_send.at[k], sum_recv.at[rank], to)

        if last:
            sums[rank] = found
            repeat(1, ranks, lambda k: sum_copy(k).start())

        def part_copy(owner, cycle=cycle):
            return send(
                weighted.at[owner + rim], parts.at[cycle, rank],
                part_send.at[cycle, owner], part_recv.at[cycle, rank], (dom, owner),
            )

        def give(owner):
            @pl.when(owner != rank)
            def _():
                part_copy(owner).start()

        repeat(rim, ranks - rim, give)

        def join(step):
            side = lax.rem(dom + 1 + step, 2)
            arrived(rim_in.at[cycle, side], rim_recv.at[cycle, side])
            base = side * (ranks - rim)
            for j in range(rim):
                weighted[rim + base + j] += rim_in[cycle, side, j]
                give(base + j)

        repeat(0, 2, join)

        near_d[cycle, reach] = weighted[rank + rim]

        def take(k):
            slot = lax.rem(rank + k, ranks)
            arrived(parts.at[cycle, slot], part_recv.at[cycle, slot])
            near_d[cycle, reach] += parts[cycle, slot]

        repeat(1, ranks, take)
        d_copies = near_copies(cycle, near_d, d_send, d_recv)
        for copy in d_copies:
            copy.start()

        def dom_copy(k):
            to = (lax.rem(dom + k, doms), rank)
            return send(dom_sums.at[dom], dom_sums.at[dom], dom_send.at[k], dom_recv.at[dom], to)

        if last:
            def take_sum(k):
                slot = lax.rem(rank + k, ranks)
                arrived(sums.at[slot], sum_recv.at[slot])

            repeat(1, ranks, take_sum)
            dom_sums[dom] = jnp.sum(sums[...], axis=0)
            repeat(1, doms, lambda k: dom_copy(k).start())

        work[...] = jnp.zeros_like(work)
        work_d[...] = jnp.zeros_like(work_d)
        for slot in range(2 * reach + 1):
            if slot != reach:
                arrived(near_h.at[cycle, slot], h_recv.at[cycle, slot])
            work[slot * planes : (slot + 1) * planes, :] = near_h[cycle, slot]
        for slot in range(2 * reach + 1):
            if slot != reach:
                arrived(near_d.at[cycle, slot], d_recv.at[cycle, slot])
            work_d[slot * planes : (slot + 1) * planes, :] = near_d[cycle, slot]

        field = work[...]
        source = FOUR_PI * work_d[...]
        height = field.shape[0]
        column = lax.broadcasted_iota(jnp.int32, field.shape, 1) % SIDE
        for _ in range(SWEEPS):
            left = jnp.where(
                column == 0, pltpu.roll(field, cells - (SIDE - 1), 1), pltpu.roll(field, 1, 1)
            )
            right = jnp.where(
                column == SIDE - 1, pltpu.roll(field, SIDE - 1, 1),
                pltpu.roll(field, cells - 1, 1),
            )
            near = pltpu.roll(field, 1, 0) + pltpu.roll(field, height - 1, 0)
            near = near + left + right
            near = near + pltpu.roll(field, SIDE, 1) + pltpu.roll(field, cells - SIDE, 1)
            field = field + RELAXATION * ((near + source) * (1.0 / 6.0) - field)
        work[...] = field
        mine = work[reach * planes : (reach + 1) * planes, :]
        density = near_d[cycle, reach]
        root = jnp.exp(jnp.log(density) * (1.0 / 3.0))
        root = root - (root - density / (root * root)) * (1.0 / 3.0)
        result = mine - EXCHANGE_FACTOR * root

        for copy in h_copies:
            copy.wait_send()
        if not last:
            slot = rank + rim
            box_pot[slot] = result

            def box_copy(k):
                to = (dom, lax.rem(rank + k, ranks))
                return send(
                    box_pot.at[rank + rim], box_pot.at[rank + rim],
                    box_send.at[k], box_recv.at[rank + rim], to,
                )

            repeat(1, ranks, lambda k: box_copy(k).start())
            near_h[cycle + 1, reach] = mine
            h_copies = near_copies(cycle + 1, near_h, h_send, h_recv)
            for copy in h_copies:
                copy.start()

            def relay_copy(index):
                side, j = lax.div(index, rim), lax.rem(index, rim)
                owner = side * (ranks - rim) + j
                target = jnp.where(side == 0, chunks - rim + j, j)
                to_dom = lax.rem(dom + jnp.where(side == 0, doms - 1, 1), doms)
                return send(
                    box_pot.at[owner + rim], box_pot.at[target],
                    relay_send.at[index], box_recv.at[target], (to_dom, rank),
                )

            def relay(index):
                side, j = lax.div(index, rim), lax.rem(index, rim)
                owner = side * (ranks - rim) + j

                @pl.when(owner != rank)
                def _():
                    arrived(box_pot.at[owner + rim], box_recv.at[owner + rim])

                relay_copy(index).start()

            repeat(0, 2 * rim, relay)

            def take_core(owner):
                @pl.when(owner != rank)
                def _():
                    arrived(box_pot.at[owner + rim], box_recv.at[owner + rim])

            def take_rim(index):
                arrived(box_pot.at[index], box_recv.at[index])
                target = rim + ranks + index
                arrived(box_pot.at[target], box_recv.at[target])

            repeat(rim, ranks - rim, take_core)
            repeat(0, rim, take_rim)
            repeat(1, ranks, lambda k: box_copy(k).wait_send())
            repeat(0, 2 * rim, lambda index: relay_copy(index).wait_send())

        for copy in rims + d_copies:
            copy.wait_send()

        def gave(owner):
            @pl.when(owner != rank)
            def _():
                part_copy(owner).wait_send()

        repeat(0, ranks, gave)
        if last:
            def take_dom(k):
                slot = lax.rem(dom + k, doms)
                arrived(dom_sums.at[slot], dom_recv.at[slot])

            repeat(1, doms, take_dom)
            total = jnp.sum(jnp.sum(dom_sums[...], axis=0), axis=0, keepdims=True)
            total = jnp.sum(total, axis=1, keepdims=True)
            average = total / (everyone * planes * cells)
            shift = (-SWEEPS * RELAXATION * FOUR_PI / 6.0) * average
            output[...] = result + shift
            repeat(1, ranks, lambda k: sum_copy(k).wait_send())
            repeat(1, doms, lambda k: dom_copy(k).wait_send())


def body(
    orbitals, occupations, occupied_count, weights, external_potential, core_density, hartree_guess
):
    doms, ranks = lax.axis_size("dom"), lax.axis_size("orb")
    count, box, cells = orbitals.shape[1:]
    planes = hartree_guess.shape[0]
    chunks = box // planes
    rim = BUF // planes
    reach = -(-SWEEPS // planes)
    span = 2 * reach + 1
    rows = -(-span * planes // 8) * 8
    shape = Segments(count, box, cells)
    lines = shape.deep * shape.lines
    f32 = jnp.float32
    anywhere = pl.BlockSpec(memory_space=pl.ANY)
    scalars = pl.BlockSpec(memory_space=pltpu.SMEM)
    dma = pltpu.SemaphoreType.DMA
    vmem = lambda *dims: pltpu.VMEM(dims, f32)
    return pl.pallas_call(
        functools.partial(cycles_kernel, doms, ranks),
        out_shape=jax.ShapeDtypeStruct((planes, cells), f32),
        in_specs=[anywhere, scalars, scalars, scalars, anywhere, anywhere, anywhere],
        out_specs=pl.BlockSpec(memory_space=pltpu.VMEM),
        scratch_shapes=[
            vmem(count, shape.tiles, box, LANES),
            vmem(shape.tiles, box, LANES),
            vmem(shape.tiles, box, LANES),
            vmem(shape.tiles, box, LANES),
            vmem(box, LANES),
            vmem(lines, SIDE + 16, LANES),
            vmem(lines, SIDE + 16, LANES),
            vmem(lines, SIDE, LANES),
            vmem(8, LANES),
            vmem(chunks, planes, cells),
            vmem(CYCLES, 2, rim, planes, cells),
            vmem(CYCLES, ranks, planes, cells),
            vmem(CYCLES, span, planes, cells),
            vmem(CYCLES, span, planes, cells),
            vmem(rows, cells),
            vmem(rows, cells),
            vmem(chunks, planes, cells),
            vmem(ranks, 8, LANES),
            vmem(doms, 8, LANES),
            dma((3 + count,)),
            dma((CYCLES, 2)), dma((CYCLES, 2)),
            dma((CYCLES, ranks)), dma((CYCLES, ranks)),
            dma((CYCLES, span)), dma((CYCLES, span)),
            dma((CYCLES, span)), dma((CYCLES, span)),
            dma((ranks,)), dma((ranks,)),
            dma((doms,)), dma((doms,)),
            dma((ranks,)), dma((chunks,)),
            dma((2 * rim,)),
        ],
        compiler_params=pltpu.CompilerParams(collective_id=0, has_side_effects=True),
        name="cycles",
    )(
        orbitals[0], occupations, occupied_count, weights, external_potential[0],
        core_density[0], hartree_guess,
    )


def solution(mesh):
    placed = (
        P("dom", "orb", None, None),
        P("dom", "orb"),
        P("dom"),
        P("dom", None),
        P("dom", None, None),
        P("dom", None, None),
        P(("dom", "orb"), None),
    )
    return jax.shard_map(
        body, mesh=mesh, in_specs=placed, out_specs=P(("dom", "orb"), None), check_vma=False
    )
```

```python
import functools

import jax
import jax.numpy as jnp
from jax import lax
from jax.experimental import pallas as pl
from jax.experimental.pallas import tpu as pltpu
from jax.sharding import PartitionSpec as P

SIDE = 48
BUF = 8
DEGREE = 8
SWEEPS = 4
CYCLES = 2
LANES = 128
HALF = 64
SEGMENTS = 4
GROUP = 4
PITCH = 72
SCALE_PITCH = 56


EXCHANGE_FACTOR = (3.0 / 3.141592653589793) ** (1.0 / 3.0)
FOUR_PI = 4.0 * 3.141592653589793
RELAXATION = 0.8
CUTOFF = 1.5


MESH = pl.DeviceIdType.MESH


class Segments:
    def __init__(self, count, box, cells):
        self.count, self.box, self.cells = count, box, cells
        self.lines = cells // SIDE // SEGMENTS
        self.across = LANES // (SEGMENTS * count)
        self.deep = box // self.across
        self.length = self.lines * SIDE
        self.tiles = cells // LANES
        self.blocks = -(-self.length // LANES)
        self.shift = count * self.across
        self.stored = (self.deep + 2) * (self.lines + 2)
        assert self.deep * self.across == box and self.length % HALF == 0
        assert self.tiles * LANES == cells and SIDE % 8 == 0 and box % 8 == 0

    def block(self, plane, line):
        return (plane + 1) * (self.lines + 2) + line + 1

    def spread(self, load, store):
        lane = lax.broadcasted_iota(jnp.int32, (self.across, LANES), 1)
        for plane in range(self.deep):
            kept = {}

            def tile_of(orbital, tile, turned):
                if (orbital, tile, turned) not in kept:
                    value = load(orbital, tile, plane)
                    kept[orbital, tile, turned] = pltpu.roll(value, HALF, 1) if turned else value
                return kept[orbital, tile, turned]

            for block in range(self.blocks):
                rows = min(LANES, self.length - block * LANES)
                pieces = []
                for segment in range(SEGMENTS):
                    first = segment * self.length + block * LANES
                    for orbital in range(self.count):
                        parts = []
                        for half in range(2):
                            cell = min(first + half * HALF, self.cells - HALF)
                            turned = cell % LANES != half * HALF
                            parts.append(tile_of(orbital, cell // LANES, turned))
                        if rows <= HALF or parts[0] is parts[1]:
                            pieces.append(parts[0])
                        else:
                            pieces.append(jnp.where(lane < HALF, parts[0], parts[1]))
                turned = jnp.concatenate(pieces, axis=0).T
                for row in range(0, rows, 8):
                    store(plane, block * LANES + row, turned[row : row + 8])

    def gather(self, load, store):
        lane = lax.broadcasted_iota(jnp.int32, (self.across, LANES), 1)
        for plane in range(self.deep):
            sums = {}
            for block in range(self.blocks):
                rows = min(LANES, self.length - block * LANES)
                pieces = [load(plane, block * LANES + row) for row in range(0, rows, 8)]
                if rows < LANES:
                    pieces.append(jnp.zeros((LANES - rows, LANES), jnp.float32))
                turned = jnp.concatenate(pieces, axis=0).T
                for segment in range(SEGMENTS):
                    base = segment * self.shift
                    value = turned[base : base + self.across]
                    for orbital in range(1, self.count):
                        at = base + orbital * self.across
                        value = value + turned[at : at + self.across]
                    sums[segment, block, False] = value

            def half_of(cell, half):
                segment, place = cell // self.length, cell % self.length
                turned = place % LANES != half * HALF
                key = (segment, place // LANES, turned)
                if key not in sums:
                    sums[key] = pltpu.roll(sums[key[0], key[1], False], HALF, 1)
                return sums[key]

            for tile in range(self.tiles):
                low = half_of(tile * LANES, 0)
                high = half_of(tile * LANES + HALF, 1)
                store(plane, tile, low if low is high else jnp.where(lane < HALF, low, high))


def put_cells(shape, target, plane, start, base, value):
    block = slice(shape.block(plane, start), shape.block(plane, start) + value.shape[0])
    target[block, 8 + base : 16 + base, :] = value
    if base == 0:
        target[block, 8 + SIDE : 9 + SIDE, :] = value[:, :1, :]
    if base == SIDE - 8:
        target[block, 7:8, :] = value[:, 7:, :]


def put_faces(shape, target, plane, start, base, value):
    lines, deep, across = shape.lines, shape.deep, shape.across
    count = value.shape[0]
    cells = slice(8 + base, 16 + base)

    def turn(part, amount):
        return pltpu.roll(part.reshape(-1, LANES), amount, 1).reshape(part.shape)

    def at(plane, line, number):
        first = shape.block(plane, line)
        return slice(first, first + number)

    lane = lax.broadcasted_iota(jnp.int32, value.shape, 2) % across
    if plane == deep - 1:
        target[at(-1, start, count), cells, :] = jnp.where(lane != 0, turn(value, 1), 0.0)
    if plane == 0:
        target[at(deep, start, count), cells, :] = jnp.where(
            lane != across - 1, turn(value, LANES - 1), 0.0
        )
    if start == 0:
        target[at(plane, lines, 1), cells, :] = turn(value[:1], LANES - shape.shift)
    if start + count == lines:
        target[at(plane, -1, 1), cells, :] = turn(value[count - 1 :], shape.shift)


def filter_step(shape, source, target, scale, inverse, first):
    lines, deep = shape.lines, shape.deep
    for base in range(0, SIDE, 8):
        cells = slice(8 + base, 16 + base)
        for start in range(0, lines, GROUP):
            grown = [
                source[shape.block(plane, start - 1) : shape.block(plane, start + GROUP + 1), cells, :]
                if 0 <= plane < deep
                else source[shape.block(plane, start) : shape.block(plane, start + GROUP), cells, :]
                for plane in range(-1, deep + 1)
            ]
            middles = [part[1:-1] if 0 < i <= deep else part for i, part in enumerate(grown)]
            for plane in range(deep):
                first_block = shape.block(plane, start)
                block = slice(first_block, first_block + GROUP)
                rows = slice(plane * lines + start, plane * lines + start + GROUP)
                middle = middles[plane + 1]
                near = source[block, 7 + base : 15 + base, :] + source[block, 9 + base : 17 + base, :]
                near = near + (grown[plane + 1][:-2] + grown[plane + 1][2:])
                near = near + (middles[plane] + middles[plane + 2])
                value = scale[rows, base : base + 8, :] * middle - inverse * near
                if first:
                    value = 0.5 * value
                else:
                    value = value - target[block, cells, :]
                put_cells(shape, target, plane, start, base, value)
                put_faces(shape, target, plane, start, base, value)


def cycles_kernel(doms, ranks, *refs):
    (
        orbitals_hbm, occupations, occupied, weights, ionic_hbm, core_hbm, hartree_hbm,
        output,
        planes_of, ionic, core, flat, weight_rows, even, odd, scale, charge,
        weighted, rim_in, parts, near_h, near_d, work, work_d, box_pot, sums, dom_sums,
        load_sem, rim_send, rim_recv, part_send, part_recv, h_send, h_recv, d_send, d_recv,
        sum_send, sum_recv, dom_send, dom_recv, box_send, box_recv, relay_send,
    ) = refs
    count, box, cells = orbitals_hbm.shape
    chunks, planes, _ = weighted.shape
    shape = Segments(count, box, cells)
    tiles = shape.tiles
    rim = BUF // planes
    span = near_h.shape[1]
    reach = span // 2
    assert planes + 2 * (SWEEPS - 2) <= 8
    everyone = doms * ranks
    dom = lax.axis_index("dom")
    rank = lax.axis_index("orb")
    me = dom * ranks + rank

    def place(index):
        return (lax.div(index, ranks), lax.rem(index, ranks))

    def send(source, target, send_sem, recv_sem, to):
        return pltpu.make_async_remote_copy(
            src_ref=source, dst_ref=target, send_sem=send_sem, recv_sem=recv_sem,
            device_id=to, device_id_type=MESH,
        )

    def repeat(low, high, step):
        lax.fori_loop(low, high, lambda i, carry: (step(i), carry)[1], 0)

    def outward(low, high, step):
        def both(i):
            pl.when(ranks - 1 - i > rank)(lambda: step(ranks - 1 - i))
            pl.when(i < rank)(lambda: step(i))

        repeat(low, high, both)

    def arrived(target, sem):
        send(target, target, sem, sem, (dom, rank)).wait_recv()

    def loads(source, target, sem):
        for tile in range(tiles):
            pltpu.make_async_copy(
                source.at[:, tile * LANES : (tile + 1) * LANES],
                target.at[tile],
                sem,
            ).start()

    def loaded(target, sem):
        pltpu.make_async_copy(target, target, sem).wait()

    loads(ionic_hbm, ionic, load_sem.at[0])
    for orbital in range(count):
        loads(orbitals_hbm.at[orbital], planes_of.at[orbital], load_sem.at[1 + orbital])
    guess = pltpu.make_async_copy(hartree_hbm, near_h.at[0, reach], load_sem.at[1 + count])
    guess.start()
    loads(core_hbm, core, load_sem.at[2 + count])

    barrier = pltpu.get_barrier_semaphore()

    def greet(k):
        pl.semaphore_signal(
            barrier, inc=1, device_id=place(lax.rem(me + k, everyone)), device_id_type=MESH
        )

    repeat(1, everyone, greet)

    sublane = lax.broadcasted_iota(jnp.int32, (8, LANES), 0)
    for group in range(0, box, 8):
        rows = jnp.full((8, LANES), weights[0, group], jnp.float32)
        for row in range(1, 8):
            rows = jnp.where(sublane == row, weights[0, group + row], rows)
        weight_rows[group : group + 8, :] = rows

    lane = lax.broadcasted_iota(jnp.int32, (8, LANES), 1)
    orbital_of = lax.rem(lax.div(lane, shape.across), count)

    def strided(ref, tile, plane):
        return ref[tile, pl.ds(plane, shape.across, stride=shape.deep), :]

    def store_orbitals(plane, cell, value):
        put_cells(shape, even, plane, cell // SIDE, cell % SIDE, value[None])

    def store_scale(plane, cell, value):
        scale[plane * shape.lines + cell // SIDE, cell % SIDE : cell % SIDE + 8, :] = value

    def near_copies(cycle, buffer, send_sems, recv_sems):
        copies = []
        for k in range(1, reach + 1):
            for sign in (1, -1):
                to = place(lax.rem(me + sign * k + everyone, everyone))
                slot = reach - sign * k
                copies.append(
                    send(
                        buffer.at[cycle, reach], buffer.at[cycle, slot],
                        send_sems.at[cycle, slot], recv_sems.at[cycle, slot], to,
                    )
                )
        return copies

    factors = []
    for orbital in range(count):
        taken = rank * count + orbital < occupied[0, 0]
        factors.append(
            jnp.where(taken, occupations[0, orbital], jnp.float32(0.0)) / (ranks * count)
        )
    norms = [jnp.float32(1.0)] * count
    h_copies = None

    for cycle in range(CYCLES):
        last = cycle + 1 == CYCLES
        if cycle == 0:
            loaded(ionic, load_sem.at[0])
            flat[...] = ionic[...]
        else:
            for tile in range(tiles):
                lanes = slice(tile * LANES, (tile + 1) * LANES)
                for group in range(0, box, 8):
                    first = group // planes
                    pieces = [box_pot[first + i, :, lanes] for i in range(8 // planes)]
                    flat[tile, group : group + 8, :] = ionic[
                        tile, group : group + 8, :
                    ] + jnp.concatenate(pieces, axis=0)
        potential = flat[...]
        lowest = jnp.min(jnp.min(potential, axis=0), axis=0, keepdims=True)
        lowest = jnp.min(lowest, axis=1, keepdims=True)
        highest = jnp.max(jnp.max(potential, axis=0), axis=0, keepdims=True)
        highest = jnp.max(highest, axis=1, keepdims=True)
        low_bound = lowest + CUTOFF
        high_bound = highest + 6.0
        center = 0.5 * (high_bound + low_bound)
        inverse = 1.0 / (0.5 * (high_bound - low_bound))
        flat[...] = (2.0 * inverse) * ((3.0 - center) + potential)
        shape.spread(lambda _, tile, plane: strided(flat, tile, plane), store_scale)
        if cycle == 0:
            for orbital in range(count):
                loaded(planes_of.at[orbital], load_sem.at[1 + orbital])
            shape.spread(
                lambda orbital, tile, plane: strided(planes_of.at[orbital], tile, plane),
                store_orbitals,
            )
            for base in range(0, SIDE, 8):
                for start in range(0, shape.lines, GROUP):
                    for plane in range(shape.deep):
                        first = shape.block(plane, start)
                        value = even[first : first + GROUP, 8 + base : 16 + base, :]
                        put_faces(shape, even, plane, start, base, value)

        filter_step(shape, even, odd, scale, inverse, True)
        if cycle == 0:
            pl.semaphore_wait(barrier, everyone - 1)
            guess.wait()
            h_copies = near_copies(0, near_h, h_send, h_recv)
            for copy in h_copies:
                copy.start()

        def two_steps(step, carry):
            filter_step(shape, odd, even, scale, inverse, False)
            filter_step(shape, even, odd, scale, inverse, False)
            return carry

        lax.fori_loop(0, (DEGREE - 1) // 2, two_steps, 0)
        filter_step(shape, odd, even, scale, inverse, False)

        total = jnp.zeros((8, LANES), jnp.float32)
        for base in range(0, SIDE, 8):
            for plane in range(shape.deep):
                value = even[
                    shape.block(plane, 0) : shape.block(plane, shape.lines), 8 + base : 16 + base, :
                ]
                total = total + jnp.sum(value * value, axis=0)
        shares = jnp.zeros((8, LANES), jnp.float32)
        for orbital in range(count):
            square = jnp.sum(
                jnp.where(orbital_of == orbital, total, 0.0), axis=0, keepdims=True
            )
            square = jnp.sum(square, axis=1, keepdims=True)
            square = norms[orbital] * square * (1.0 / (box * cells)) + 1e-06
            share = factors[orbital] * norms[orbital] / square
            shares = jnp.where(orbital_of == orbital, share, shares)
            norms[orbital] = norms[orbital] / square

        def load_density(plane, cell):
            at = cell % SIDE
            value = even[shape.block(plane, cell // SIDE), 8 + at : 16 + at, :]
            return shares * (value * value)

        def store_density(plane, tile, value):
            flat[tile, pl.ds(plane, shape.across, stride=shape.deep), :] = value

        shape.gather(load_density, store_density)
        if cycle == 0:
            loaded(core, load_sem.at[2 + count])
        found = jnp.zeros((8, LANES), jnp.float32) if cycle == 0 else charge[...]
        for group in range(0, box, 8):
            rows = slice(group, group + 8)
            weight = weight_rows[rows, :]
            for tile in range(tiles):
                density = flat[tile, rows, :] + core[tile, rows, :] * (1.0 / ranks)
                density = density * weight
                found = found + density
                for piece in range(8 // planes):
                    weighted[
                        group // planes + piece, :, tile * LANES : (tile + 1) * LANES
                    ] = density[piece * planes : (piece + 1) * planes]
        charge[...] = found

        down = (lax.rem(dom + doms - 1, doms), rank)
        up = (lax.rem(dom + 1, doms), rank)
        rims = [
            send(
                weighted.at[:rim], rim_in.at[cycle, 1],
                rim_send.at[cycle, 1], rim_recv.at[cycle, 1], down,
            ),
            send(
                weighted.at[rim + ranks :], rim_in.at[cycle, 0],
                rim_send.at[cycle, 0], rim_recv.at[cycle, 0], up,
            ),
        ]
        for copy in rims:
            copy.start()

        def sum_copy(k):
            to = (dom, lax.rem(rank + k, ranks))
            return send(sums.at[rank], sums.at[rank], sum_send.at[k], sum_recv.at[rank], to)

        if last:
            sums[rank] = found
            repeat(1, ranks, lambda k: sum_copy(k).start())

        def part_copy(owner, cycle=cycle):
            return send(
                weighted.at[owner + rim], parts.at[cycle, rank],
                part_send.at[cycle, owner], part_recv.at[cycle, rank], (dom, owner),
            )

        def give(owner):
            part_copy(owner).start()

        outward(rim, ranks - rim, give)

        def join(step):
            side = lax.rem(dom + 1 + step, 2)
            arrived(rim_in.at[cycle, side], rim_recv.at[cycle, side])
            base = side * (ranks - rim)
            for j in range(rim):
                weighted[rim + base + j] += rim_in[cycle, side, j]
                pl.when(base + j != rank)(lambda: give(base + j))

        repeat(0, 2, join)

        near_d[cycle, reach] = weighted[rank + rim]

        def take(k):
            slot = lax.rem(rank + k, ranks)
            arrived(parts.at[cycle, slot], part_recv.at[cycle, slot])
            near_d[cycle, reach] += parts[cycle, slot]

        repeat(1, ranks, take)
        d_copies = near_copies(cycle, near_d, d_send, d_recv)
        for copy in d_copies:
            copy.start()

        def dom_copy(k):
            to = (lax.rem(dom + k, doms), rank)
            return send(dom_sums.at[dom], dom_sums.at[dom], dom_send.at[k], dom_recv.at[dom], to)

        if last:
            def take_sum(k):
                slot = lax.rem(rank + k, ranks)
                arrived(sums.at[slot], sum_recv.at[slot])

            repeat(1, ranks, take_sum)
            dom_sums[dom] = jnp.sum(sums[...], axis=0)
            repeat(1, doms, lambda k: dom_copy(k).start())

        height = work.shape[0]
        origin = reach * planes - 2

        def put(target, slot, value):
            run = min(planes, 2)
            for row in range(0, planes, run):
                at = (slot * planes + row - origin) % height
                target[at : at + run, :] = value[row : row + run]

        if span * planes < height:
            work[...] = jnp.zeros_like(work)
            work_d[...] = jnp.zeros_like(work_d)
        for slot in range(span):
            if slot != reach:
                arrived(near_h.at[cycle, slot], h_recv.at[cycle, slot])
            put(work, slot, near_h[cycle, slot])
        for slot in range(span):
            if slot != reach:
                arrived(near_d.at[cycle, slot], d_recv.at[cycle, slot])
            put(work_d, slot, near_d[cycle, slot])

        field = work[...]
        source = FOUR_PI * work_d[...]
        column = lax.broadcasted_iota(jnp.int32, field.shape, 1) % SIDE
        for sweep in range(SWEEPS):
            near = pltpu.roll(field, 1, 0) + pltpu.roll(field, field.shape[0] - 1, 0)
            if sweep == 1:
                field, near, source, column = field[:8], near[:8], source[:8], column[:8]
            left = jnp.where(
                column == 0, pltpu.roll(field, cells - (SIDE - 1), 1), pltpu.roll(field, 1, 1)
            )
            right = jnp.where(
                column == SIDE - 1, pltpu.roll(field, SIDE - 1, 1),
                pltpu.roll(field, cells - 1, 1),
            )
            near = near + left + right
            near = near + pltpu.roll(field, SIDE, 1) + pltpu.roll(field, cells - SIDE, 1)
            field = field + RELAXATION * ((near + source) * (1.0 / 6.0) - field)
        work[:8, :] = field
        mine = work[2 : 2 + planes, :]
        density = near_d[cycle, reach]
        root = jnp.exp(jnp.log(density) * (1.0 / 3.0))
        root = root - (root - density / (root * root)) * (1.0 / 3.0)
        result = mine - EXCHANGE_FACTOR * root

        for copy in h_copies:
            copy.wait_send()
        if not last:
            slot = rank + rim
            box_pot[slot] = result

            def box_copy(to):
                return send(
                    box_pot.at[rank + rim], box_pot.at[rank + rim],
                    box_send.at[to], box_recv.at[rank + rim], (dom, to),
                )

            outward(0, ranks, lambda to: box_copy(to).start())
            near_h[cycle + 1, reach] = mine
            h_copies = near_copies(cycle + 1, near_h, h_send, h_recv)
            for copy in h_copies:
                copy.start()

            def relay_copy(index):
                side, j = lax.div(index, rim), lax.rem(index, rim)
                owner = side * (ranks - rim) + j
                target = jnp.where(side == 0, chunks - rim + j, j)
                to_dom = lax.rem(dom + jnp.where(side == 0, doms - 1, 1), doms)
                return send(
                    box_pot.at[owner + rim], box_pot.at[target],
                    relay_send.at[index], box_recv.at[target], (to_dom, rank),
                )

            def relay(step):
                index = lax.rem(step + jnp.where(2 * rank < ranks, 0, rim), 2 * rim)
                side, j = lax.div(index, rim), lax.rem(index, rim)
                owner = side * (ranks - rim) + j

                @pl.when(owner != rank)
                def _():
                    arrived(box_pot.at[owner + rim], box_recv.at[owner + rim])

                relay_copy(index).start()

            repeat(0, 2 * rim, relay)

            def take_core(owner):
                @pl.when(owner != rank)
                def _():
                    arrived(box_pot.at[owner + rim], box_recv.at[owner + rim])

            def take_rim(index):
                arrived(box_pot.at[index], box_recv.at[index])
                target = rim + ranks + index
                arrived(box_pot.at[target], box_recv.at[target])

            repeat(rim, ranks - rim, take_core)
            repeat(0, rim, take_rim)
            outward(0, ranks, lambda to: box_copy(to).wait_send())
            repeat(0, 2 * rim, lambda index: relay_copy(index).wait_send())

        for copy in rims + d_copies:
            copy.wait_send()

        outward(0, ranks, lambda owner: part_copy(owner).wait_send())
        if last:
            def take_dom(k):
                slot = lax.rem(dom + k, doms)
                arrived(dom_sums.at[slot], dom_recv.at[slot])

            repeat(1, doms, take_dom)
            total = jnp.sum(jnp.sum(dom_sums[...], axis=0), axis=0, keepdims=True)
            total = jnp.sum(total, axis=1, keepdims=True)
            average = total / (everyone * planes * cells)
            shift = (-SWEEPS * RELAXATION * FOUR_PI / 6.0) * average
            output[...] = result + shift
            repeat(1, ranks, lambda k: sum_copy(k).wait_send())
            repeat(1, doms, lambda k: dom_copy(k).wait_send())


def body(
    orbitals, occupations, occupied_count, weights, external_potential, core_density, hartree_guess
):
    doms, ranks = lax.axis_size("dom"), lax.axis_size("orb")
    count, box, cells = orbitals.shape[1:]
    planes = hartree_guess.shape[0]
    chunks = box // planes
    rim = BUF // planes
    reach = -(-SWEEPS // planes)
    span = 2 * reach + 1
    rows = -(-span * planes // 8) * 8
    shape = Segments(count, box, cells)
    lines = shape.deep * shape.lines
    f32 = jnp.float32
    anywhere = pl.BlockSpec(memory_space=pl.ANY)
    scalars = pl.BlockSpec(memory_space=pltpu.SMEM)
    dma = pltpu.SemaphoreType.DMA
    vmem = lambda *dims: pltpu.VMEM(dims, f32)
    return pl.pallas_call(
        functools.partial(cycles_kernel, doms, ranks),
        out_shape=pltpu.VMEM((planes, cells), f32),
        in_specs=[anywhere, scalars, scalars, scalars, anywhere, anywhere, anywhere],
        out_specs=pl.BlockSpec(memory_space=pltpu.VMEM),
        scratch_shapes=[
            vmem(count, shape.tiles, box, LANES),
            vmem(shape.tiles, box, LANES),
            vmem(shape.tiles, box, LANES),
            vmem(shape.tiles, box, LANES),
            vmem(box, LANES),
            vmem(shape.stored, PITCH, LANES),
            vmem(shape.stored, PITCH, LANES),
            vmem(lines, SCALE_PITCH, LANES),
            vmem(8, LANES),
            vmem(chunks, planes, cells),
            vmem(CYCLES, 2, rim, planes, cells),
            vmem(CYCLES, ranks, planes, cells),
            vmem(CYCLES, span, planes, cells),
            vmem(CYCLES, span, planes, cells),
            vmem(rows, cells),
            vmem(rows, cells),
            vmem(chunks, planes, cells),
            vmem(ranks, 8, LANES),
            vmem(doms, 8, LANES),
            dma((3 + count,)),
            dma((CYCLES, 2)), dma((CYCLES, 2)),
            dma((CYCLES, ranks)), dma((CYCLES, ranks)),
            dma((CYCLES, span)), dma((CYCLES, span)),
            dma((CYCLES, span)), dma((CYCLES, span)),
            dma((ranks,)), dma((ranks,)),
            dma((doms,)), dma((doms,)),
            dma((ranks,)), dma((chunks,)),
            dma((2 * rim,)),
        ],
        compiler_params=pltpu.CompilerParams(collective_id=0, has_side_effects=True),
        name="cycles",
    )(
        orbitals[0], occupations, occupied_count.reshape(1, 1), weights, external_potential[0],
        core_density[0], hartree_guess,
    )


def solution(mesh):
    placed = (
        P("dom", "orb", None, None),
        P("dom", "orb"),
        P("dom"),
        P("dom", None),
        P("dom", None, None),
        P("dom", None, None),
        P(("dom", "orb"), None),
    )
    return jax.shard_map(
        body, mesh=mesh, in_specs=placed, out_specs=P(("dom", "orb"), None), check_vma=False
    )
```

```python
import functools

import jax
import jax.numpy as jnp
from jax import lax
from jax.experimental import pallas as pl
from jax.experimental.pallas import tpu as pltpu
from jax.sharding import PartitionSpec as P

SIDE = 48
BUF = 8
DEGREE = 8
SWEEPS = 4
CYCLES = 2
LANES = 128
HALF = 64
SEGMENTS = 4
GROUP = 4
PITCH = 72
SCALE_PITCH = 56


EXCHANGE_FACTOR = (3.0 / 3.141592653589793) ** (1.0 / 3.0)
FOUR_PI = 4.0 * 3.141592653589793
RELAXATION = 0.8
CUTOFF = 1.5


MESH = pl.DeviceIdType.MESH


class Segments:
    def __init__(self, count, box, cells):
        self.count, self.box, self.cells = count, box, cells
        self.lines = cells // SIDE // SEGMENTS
        self.across = LANES // (SEGMENTS * count)
        self.deep = box // self.across
        self.length = self.lines * SIDE
        self.tiles = cells // LANES
        self.blocks = -(-self.length // LANES)
        self.shift = count * self.across
        self.stored = (self.deep + 2) * (self.lines + 2)
        assert self.deep * self.across == box and self.length % HALF == 0
        assert self.tiles * LANES == cells and SIDE % 8 == 0 and box % 8 == 0

    def block(self, plane, line):
        return (plane + 1) * (self.lines + 2) + line + 1

    def spread(self, load, store):
        lane = lax.broadcasted_iota(jnp.int32, (self.across, LANES), 1)
        for plane in range(self.deep):
            kept = {}

            def tile_of(orbital, tile, turned):
                if (orbital, tile, turned) not in kept:
                    value = load(orbital, tile, plane)
                    kept[orbital, tile, turned] = pltpu.roll(value, HALF, 1) if turned else value
                return kept[orbital, tile, turned]

            for block in range(self.blocks):
                rows = min(LANES, self.length - block * LANES)
                pieces = []
                for segment in range(SEGMENTS):
                    first = segment * self.length + block * LANES
                    for orbital in range(self.count):
                        parts = []
                        for half in range(2):
                            cell = min(first + half * HALF, self.cells - HALF)
                            turned = cell % LANES != half * HALF
                            parts.append(tile_of(orbital, cell // LANES, turned))
                        if rows <= HALF or parts[0] is parts[1]:
                            pieces.append(parts[0])
                        else:
                            pieces.append(jnp.where(lane < HALF, parts[0], parts[1]))
                turned = jnp.concatenate(pieces, axis=0).T
                for row in range(0, rows, 8):
                    store(plane, block * LANES + row, turned[row : row + 8])

    def gather(self, load, store):
        lane = lax.broadcasted_iota(jnp.int32, (self.across, LANES), 1)
        for plane in range(self.deep):
            sums = {}
            for block in range(self.blocks):
                rows = min(LANES, self.length - block * LANES)
                pieces = [load(plane, block * LANES + row) for row in range(0, rows, 8)]
                if rows < LANES:
                    pieces.append(jnp.zeros((LANES - rows, LANES), jnp.float32))
                turned = jnp.concatenate(pieces, axis=0).T
                for segment in range(SEGMENTS):
                    base = segment * self.shift
                    value = turned[base : base + self.across]
                    for orbital in range(1, self.count):
                        at = base + orbital * self.across
                        value = value + turned[at : at + self.across]
                    sums[segment, block, False] = value

            def half_of(cell, half):
                segment, place = cell // self.length, cell % self.length
                turned = place % LANES != half * HALF
                key = (segment, place // LANES, turned)
                if key not in sums:
                    sums[key] = pltpu.roll(sums[key[0], key[1], False], HALF, 1)
                return sums[key]

            for tile in range(self.tiles):
                low = half_of(tile * LANES, 0)
                high = half_of(tile * LANES + HALF, 1)
                store(plane, tile, low if low is high else jnp.where(lane < HALF, low, high))


def put_cells(shape, target, plane, start, base, value):
    block = slice(shape.block(plane, start), shape.block(plane, start) + value.shape[0])
    target[block, 8 + base : 16 + base, :] = value
    if base == 0:
        target[block, 8 + SIDE : 9 + SIDE, :] = value[:, :1, :]
    if base == SIDE - 8:
        target[block, 7:8, :] = value[:, 7:, :]


def put_faces(shape, target, plane, start, base, value):
    lines, deep, across = shape.lines, shape.deep, shape.across
    count = value.shape[0]
    cells = slice(8 + base, 16 + base)

    def turn(part, amount):
        return pltpu.roll(part.reshape(-1, LANES), amount, 1).reshape(part.shape)

    def at(plane, line, number):
        first = shape.block(plane, line)
        return slice(first, first + number)

    lane = lax.broadcasted_iota(jnp.int32, value.shape, 2) % across
    if plane == deep - 1:
        target[at(-1, start, count), cells, :] = jnp.where(lane != 0, turn(value, 1), 0.0)
    if plane == 0:
        target[at(deep, start, count), cells, :] = jnp.where(
            lane != across - 1, turn(value, LANES - 1), 0.0
        )
    if start == 0:
        target[at(plane, lines, 1), cells, :] = turn(value[:1], LANES - shape.shift)
    if start + count == lines:
        target[at(plane, -1, 1), cells, :] = turn(value[count - 1 :], shape.shift)


def filter_step(shape, source, target, scale, inverse, first):
    lines, deep = shape.lines, shape.deep
    for base in range(0, SIDE, 8):
        cells = slice(8 + base, 16 + base)
        for start in range(0, lines, GROUP):
            grown = [
                source[shape.block(plane, start - 1) : shape.block(plane, start + GROUP + 1), cells, :]
                if 0 <= plane < deep
                else source[shape.block(plane, start) : shape.block(plane, start + GROUP), cells, :]
                for plane in range(-1, deep + 1)
            ]
            middles = [part[1:-1] if 0 < i <= deep else part for i, part in enumerate(grown)]
            for plane in range(deep):
                first_block = shape.block(plane, start)
                block = slice(first_block, first_block + GROUP)
                rows = slice(plane * lines + start, plane * lines + start + GROUP)
                middle = middles[plane + 1]
                near = source[block, 7 + base : 15 + base, :] + source[block, 9 + base : 17 + base, :]
                near = near + (grown[plane + 1][:-2] + grown[plane + 1][2:])
                near = near + (middles[plane] + middles[plane + 2])
                value = scale[rows, base : base + 8, :] * middle - inverse * near
                if first:
                    value = 0.5 * value
                else:
                    value = value - target[block, cells, :]
                put_cells(shape, target, plane, start, base, value)
                put_faces(shape, target, plane, start, base, value)


def cycles_kernel(doms, ranks, *refs):
    (
        orbitals_hbm, occupations, occupied, weights, ionic_hbm, core_hbm, hartree_hbm,
        output,
        planes_of, ionic, core, flat, weight_rows, even, odd, scale, charge,
        weighted, rim_in, parts, near_h, near_d, work, relaxed, grown, local, box_pot, sums, dom_sums,
        load_sem, rim_send, rim_recv, part_send, part_recv, h_send, h_recv, d_send, d_recv,
        sum_send, sum_recv, dom_send, dom_recv, box_send, box_recv, relay_send,
    ) = refs
    count, box, cells = orbitals_hbm.shape
    chunks, planes, _ = weighted.shape
    shape = Segments(count, box, cells)
    tiles = shape.tiles
    rim = BUF // planes
    span = near_h.shape[1]
    reach = span // 2
    assert planes + 2 * (SWEEPS - 2) <= 8
    everyone = doms * ranks
    dom = lax.axis_index("dom")
    rank = lax.axis_index("orb")
    me = dom * ranks + rank

    def place(index):
        return (lax.div(index, ranks), lax.rem(index, ranks))

    def send(source, target, send_sem, recv_sem, to):
        return pltpu.make_async_remote_copy(
            src_ref=source, dst_ref=target, send_sem=send_sem, recv_sem=recv_sem,
            device_id=to, device_id_type=MESH,
        )

    def repeat(low, high, step):
        lax.fori_loop(low, high, lambda i, carry: (step(i), carry)[1], 0)

    def outward(low, high, step):
        def both(i):
            pl.when(ranks - 1 - i > rank)(lambda: step(ranks - 1 - i))
            pl.when(i < rank)(lambda: step(i))

        repeat(low, high, both)

    def arrived(target, sem):
        send(target, target, sem, sem, (dom, rank)).wait_recv()

    def left(source, sem):
        send(source, source, sem, sem, (dom, rank)).wait_send()

    def loads(source, target, sem):
        for tile in range(tiles):
            pltpu.make_async_copy(
                source.at[:, tile * LANES : (tile + 1) * LANES],
                target.at[tile],
                sem,
            ).start()

    def loaded(target, sem):
        pltpu.make_async_copy(target, target, sem).wait()

    loads(ionic_hbm, ionic, load_sem.at[0])
    for orbital in range(count):
        loads(orbitals_hbm.at[orbital], planes_of.at[orbital], load_sem.at[1])
    guess = pltpu.make_async_copy(hartree_hbm, near_h.at[0, reach], load_sem.at[2])
    guess.start()
    loads(core_hbm, core, load_sem.at[3])

    barrier = pltpu.get_barrier_semaphore()

    def greet(k):
        pl.semaphore_signal(
            barrier, inc=1, device_id=place(lax.rem(me + k, everyone)), device_id_type=MESH
        )

    repeat(1, everyone, greet)

    sublane = lax.broadcasted_iota(jnp.int32, (8, LANES), 0)
    for group in range(0, box, 8):
        rows = jnp.full((8, LANES), weights[0, group], jnp.float32)
        for row in range(1, 8):
            rows = jnp.where(sublane == row, weights[0, group + row], rows)
        weight_rows[group : group + 8, :] = rows

    lane = lax.broadcasted_iota(jnp.int32, (8, LANES), 1)
    orbital_of = lax.rem(lax.div(lane, shape.across), count)

    def strided(ref, tile, plane):
        return ref[tile, pl.ds(plane, shape.across, stride=shape.deep), :]

    def store_orbitals(plane, cell, value):
        put_cells(shape, even, plane, cell // SIDE, cell % SIDE, value[None])

    def store_scale(plane, cell, value):
        scale[plane * shape.lines + cell // SIDE, cell % SIDE : cell % SIDE + 8, :] = value

    def near_copies(cycle, buffer, send_sems, recv_sems):
        copies = []
        for k in range(1, reach + 1):
            for sign in (1, -1):
                to = place(lax.rem(me + sign * k + everyone, everyone))
                slot = reach - sign * k
                copies.append(
                    send(
                        buffer.at[cycle, reach], buffer.at[cycle, slot],
                        send_sems.at[cycle], recv_sems.at[cycle], to,
                    )
                )
        return copies

    factors = []
    for orbital in range(count):
        taken = rank * count + orbital < occupied[0, 0]
        factors.append(
            jnp.where(taken, occupations[0, orbital], jnp.float32(0.0)) / (ranks * count)
        )
    norms = [jnp.float32(1.0)] * count
    height = work.shape[0]
    origin = reach * planes - 2

    def put(target, slot, value):
        run = min(planes, 2)
        for row in range(0, planes, run):
            at = (slot * planes + row - origin) % height
            target[at : at + run, :] = value[row : row + run]

    def relax(field, added):
        for sweep in range(SWEEPS):
            if field is None:
                field = added
                continue
            near = pltpu.roll(field, 1, 0) + pltpu.roll(field, field.shape[0] - 1, 0)
            if sweep == 1:
                field, near = field[:8], near[:8]
            column = lax.broadcasted_iota(jnp.int32, field.shape, 1) % SIDE
            left = jnp.where(
                column == 0, pltpu.roll(field, cells - (SIDE - 1), 1), pltpu.roll(field, 1, 1)
            )
            right = jnp.where(
                column == SIDE - 1, pltpu.roll(field, SIDE - 1, 1),
                pltpu.roll(field, cells - 1, 1),
            )
            near = near + left + right
            near = near + pltpu.roll(field, SIDE, 1) + pltpu.roll(field, cells - SIDE, 1)
            field = field + RELAXATION * (near * (1.0 / 6.0) - field)
            if added is not None:
                field = field + added[: field.shape[0]]
        return field

    work[...] = jnp.zeros_like(work)
    h_copies = None

    for cycle in range(CYCLES):
        last = cycle + 1 == CYCLES
        if cycle == 0:
            loaded(ionic, load_sem.at[0])
            flat[...] = ionic[...]
        else:
            for tile in range(tiles):
                lanes = slice(tile * LANES, (tile + 1) * LANES)
                for group in range(0, box, 8):
                    first = group // planes
                    pieces = [box_pot[first + i, :, lanes] for i in range(8 // planes)]
                    flat[tile, group : group + 8, :] = ionic[
                        tile, group : group + 8, :
                    ] + jnp.concatenate(pieces, axis=0)
        potential = flat[...]
        lowest = jnp.min(jnp.min(potential, axis=0), axis=0, keepdims=True)
        lowest = jnp.min(lowest, axis=1, keepdims=True)
        highest = jnp.max(jnp.max(potential, axis=0), axis=0, keepdims=True)
        highest = jnp.max(highest, axis=1, keepdims=True)
        low_bound = lowest + CUTOFF
        high_bound = highest + 6.0
        center = 0.5 * (high_bound + low_bound)
        inverse = 1.0 / (0.5 * (high_bound - low_bound))
        flat[...] = (2.0 * inverse) * ((3.0 - center) + potential)
        shape.spread(lambda _, tile, plane: strided(flat, tile, plane), store_scale)
        if cycle == 0:
            loaded(planes_of, load_sem.at[1])
            shape.spread(
                lambda orbital, tile, plane: strided(planes_of.at[orbital], tile, plane),
                store_orbitals,
            )
            for base in range(0, SIDE, 8):
                for start in range(0, shape.lines, GROUP):
                    for plane in range(shape.deep):
                        first = shape.block(plane, start)
                        value = even[first : first + GROUP, 8 + base : 16 + base, :]
                        put_faces(shape, even, plane, start, base, value)

        filter_step(shape, even, odd, scale, inverse, True)
        if cycle == 0:
            pl.semaphore_wait(barrier, everyone - 1)
            guess.wait()
            h_copies = near_copies(0, near_h, h_send, h_recv)
            for copy in h_copies:
                copy.start()

        def two_steps(step, carry):
            filter_step(shape, odd, even, scale, inverse, False)
            filter_step(shape, even, odd, scale, inverse, False)
            return carry

        lax.fori_loop(0, (DEGREE - 1) // 2, two_steps, 0)
        filter_step(shape, odd, even, scale, inverse, False)

        total = jnp.zeros((8, LANES), jnp.float32)
        for base in range(0, SIDE, 8):
            for plane in range(shape.deep):
                value = even[
                    shape.block(plane, 0) : shape.block(plane, shape.lines), 8 + base : 16 + base, :
                ]
                total = total + jnp.sum(value * value, axis=0)
        shares = jnp.zeros((8, LANES), jnp.float32)
        for orbital in range(count):
            square = jnp.sum(
                jnp.where(orbital_of == orbital, total, 0.0), axis=0, keepdims=True
            )
            square = jnp.sum(square, axis=1, keepdims=True)
            square = norms[orbital] * square * (1.0 / (box * cells)) + 1e-06
            share = factors[orbital] * norms[orbital] / square
            shares = jnp.where(orbital_of == orbital, share, shares)
            norms[orbital] = norms[orbital] / square

        def load_density(plane, cell):
            at = cell % SIDE
            value = even[shape.block(plane, cell // SIDE), 8 + at : 16 + at, :]
            return shares * (value * value)

        def store_density(plane, tile, value):
            flat[tile, pl.ds(plane, shape.across, stride=shape.deep), :] = value

        shape.gather(load_density, store_density)
        if cycle == 0:
            loaded(core, load_sem.at[3])
        def weigh(groups, found):
            for group in groups:
                rows = slice(group, group + 8)
                weight = weight_rows[rows, :]
                for tile in range(tiles):
                    density = flat[tile, rows, :] + core[tile, rows, :] * (1.0 / ranks)
                    density = density * weight
                    found = found + density
                    for piece in range(8 // planes):
                        weighted[
                            group // planes + piece, :, tile * LANES : (tile + 1) * LANES
                        ] = density[piece * planes : (piece + 1) * planes]
            return found

        outer = list(range(0, BUF, 8)) + list(range(box - BUF, box, 8))
        edges = list(range(BUF, 2 * BUF, 8)) + list(range(box - 2 * BUF, box - BUF, 8))
        found = jnp.zeros((8, LANES), jnp.float32) if cycle == 0 else charge[...]
        found = weigh(outer, found)
        down = (lax.rem(dom + doms - 1, doms), rank)
        up = (lax.rem(dom + 1, doms), rank)
        rims = [
            send(
                weighted.at[:rim], rim_in.at[cycle, 1],
                rim_send.at[cycle], rim_recv.at[cycle, 1], down,
            ),
            send(
                weighted.at[rim + ranks :], rim_in.at[cycle, 0],
                rim_send.at[cycle], rim_recv.at[cycle, 0], up,
            ),
        ]
        for copy in rims:
            copy.start()
        found = weigh([g for g in range(2 * BUF, box - 2 * BUF, 8)], found)

        def sum_copy(k):
            to = (dom, lax.rem(rank + k, ranks))
            return send(sums.at[rank], sums.at[rank], sum_send.at[0], sum_recv.at[0], to)

        def part_copy(owner, cycle=cycle):
            return send(
                weighted.at[owner + rim], parts.at[cycle, rank],
                part_send.at[cycle], part_recv.at[cycle], (dom, owner),
            )

        def give(owner):
            part_copy(owner).start()

        outward(rim, ranks - rim, give)
        found = weigh(edges, found)
        if last:
            sums[rank] = found
            repeat(1, ranks, lambda k: sum_copy(k).start())
        else:
            charge[...] = found

        def join(step):
            side = lax.rem(dom + 1 + step, 2)
            arrived(rim_in.at[cycle, side], rim_recv.at[cycle, side])
            base = side * (ranks - rim)
            for j in range(rim):
                weighted[rim + base + j] += rim_in[cycle, side, j]
                pl.when(base + j != rank)(lambda: give(base + j))

        repeat(0, 2, join)

        arrived(near_h.at[cycle, : span - 1], h_recv.at[cycle])
        for slot in range(span):
            put(work, slot, near_h[cycle, slot])
        relaxed[...] = relax(work[...], None)

        def dom_copy(k):
            to = (lax.rem(dom + k, doms), rank)
            return send(dom_sums.at[dom], dom_sums.at[dom], dom_send.at[0], dom_recv.at[0], to)

        arrived(parts.at[cycle, : ranks - 1], part_recv.at[cycle])
        density = weighted[rank + rim]
        for k in range(1, ranks):
            density = density + parts[cycle, lax.rem(rank + k, ranks)]
        near_d[cycle, reach] = density
        d_copies = near_copies(cycle, near_d, d_send, d_recv)
        for copy in d_copies:
            copy.start()

        if last:
            arrived(sums.at[: ranks - 1], sum_recv.at[0])
            dom_sums[dom] = jnp.sum(sums[...], axis=0)
            repeat(1, doms, lambda k: dom_copy(k).start())

        root = jnp.exp(jnp.log(density) * (1.0 / 3.0))
        root = root - (root - density / (root * root)) * (1.0 / 3.0)
        local[...] = relaxed[2 : 2 + planes, :] - EXCHANGE_FACTOR * root
        arrived(near_d.at[cycle, : span - 1], d_recv.at[cycle])
        for slot in range(span):
            put(work, slot, near_d[cycle, slot])
        if last:
            arrived(dom_sums.at[: doms - 1], dom_recv.at[0])
            total = jnp.sum(jnp.sum(dom_sums[...], axis=0), axis=0, keepdims=True)
            total = jnp.sum(total, axis=1, keepdims=True)
            average = total / (everyone * planes * cells)
            shift = (-SWEEPS * RELAXATION * FOUR_PI / 6.0) * average
            local[...] += shift
        change = relax(None, (RELAXATION * FOUR_PI / 6.0) * work[...])
        grown[...] = change
        change = grown[2 : 2 + planes, :]
        result = local[...] + change

        left(near_h.at[cycle, : span - 1], h_send.at[cycle])
        if not last:
            slot = rank + rim
            box_pot[slot] = result

            late = jnp.where(rank >= ranks - rim, rank - (ranks - 2 * rim), 2 * rim)
            box_sem = jnp.where(rank < rim, rank, late)

            def box_copy(to):
                return send(
                    box_pot.at[rank + rim], box_pot.at[rank + rim],
                    box_send.at[0], box_recv.at[box_sem], (dom, to),
                )

            outward(0, ranks, lambda to: box_copy(to).start())
            near_h[cycle + 1, reach] = relaxed[2 : 2 + planes, :] + change
            h_copies = near_copies(cycle + 1, near_h, h_send, h_recv)
            for copy in h_copies:
                copy.start()

            def relay_copy(index):
                side, j = lax.div(index, rim), lax.rem(index, rim)
                owner = side * (ranks - rim) + j
                target = jnp.where(side == 0, chunks - rim + j, j)
                to_dom = lax.rem(dom + jnp.where(side == 0, doms - 1, 1), doms)
                return send(
                    box_pot.at[owner + rim], box_pot.at[target],
                    relay_send.at[0], box_recv.at[2 * rim], (to_dom, rank),
                )

            def relay(step):
                index = lax.rem(step + rim * lax.rem(dom + 1, 2), 2 * rim)
                side, j = lax.div(index, rim), lax.rem(index, rim)
                owner = side * (ranks - rim) + j

                @pl.when(owner != rank)
                def _():
                    arrived(box_pot.at[owner + rim], box_recv.at[index])

                relay_copy(index).start()

            repeat(0, 2 * rim, relay)
            at_edge = box_sem < 2 * rim

            @pl.when(at_edge)
            def _():
                arrived(box_pot.at[:ranks], box_recv.at[2 * rim])

            @pl.when(jnp.logical_not(at_edge))
            def _():
                arrived(box_pot.at[: ranks - 1], box_recv.at[2 * rim])

            left(box_pot.at[: ranks - 1], box_send.at[0])
            left(box_pot.at[: 2 * rim], relay_send.at[0])

        left(rim_in.at[cycle], rim_send.at[cycle])
        left(near_d.at[cycle, : span - 1], d_send.at[cycle])
        left(parts.at[cycle, : ranks - 1], part_send.at[cycle])
        if last:
            output[...] = result
            left(sums.at[: ranks - 1], sum_send.at[0])
            left(dom_sums.at[: doms - 1], dom_send.at[0])


def body(
    orbitals, occupations, occupied_count, weights, external_potential, core_density, hartree_guess
):
    doms, ranks = lax.axis_size("dom"), lax.axis_size("orb")
    count, box, cells = orbitals.shape[1:]
    planes = hartree_guess.shape[0]
    chunks = box // planes
    rim = BUF // planes
    reach = -(-SWEEPS // planes)
    span = 2 * reach + 1
    rows = -(-span * planes // 8) * 8
    shape = Segments(count, box, cells)
    lines = shape.deep * shape.lines
    f32 = jnp.float32
    anywhere = pl.BlockSpec(memory_space=pl.ANY)
    scalars = pl.BlockSpec(memory_space=pltpu.SMEM)
    dma = pltpu.SemaphoreType.DMA
    vmem = lambda *dims: pltpu.VMEM(dims, f32)
    return pl.pallas_call(
        functools.partial(cycles_kernel, doms, ranks),
        out_shape=pltpu.VMEM((planes, cells), f32),
        in_specs=[anywhere, scalars, scalars, scalars, anywhere, anywhere, anywhere],
        out_specs=pl.BlockSpec(memory_space=pltpu.VMEM),
        scratch_shapes=[
            vmem(count, shape.tiles, box, LANES),
            vmem(shape.tiles, box, LANES),
            vmem(shape.tiles, box, LANES),
            vmem(shape.tiles, box, LANES),
            vmem(box, LANES),
            vmem(shape.stored, PITCH, LANES),
            vmem(shape.stored, PITCH, LANES),
            vmem(lines, SCALE_PITCH, LANES),
            vmem(8, LANES),
            vmem(chunks, planes, cells),
            vmem(CYCLES, 2, rim, planes, cells),
            vmem(CYCLES, ranks, planes, cells),
            vmem(CYCLES, span, planes, cells),
            vmem(CYCLES, span, planes, cells),
            vmem(rows, cells),
            vmem(8, cells),
            vmem(8, cells),
            vmem(planes, cells),
            vmem(chunks, planes, cells),
            vmem(ranks, 8, LANES),
            vmem(doms, 8, LANES),
            dma((4,)),
            dma((CYCLES,)), dma((CYCLES, 2)),
            dma((CYCLES,)), dma((CYCLES,)),
            dma((CYCLES,)), dma((CYCLES,)),
            dma((CYCLES,)), dma((CYCLES,)),
            dma((1,)), dma((1,)),
            dma((1,)), dma((1,)),
            dma((1,)), dma((2 * rim + 1,)),
            dma((1,)),
        ],
        compiler_params=pltpu.CompilerParams(collective_id=0, has_side_effects=True),
        name="cycles",
    )(
        orbitals[0], occupations, occupied_count.reshape(1, 1), weights, external_potential[0],
        core_density[0], hartree_guess,
    )


def solution(mesh):
    placed = (
        P("dom", "orb", None, None),
        P("dom", "orb"),
        P("dom"),
        P("dom", None),
        P("dom", None, None),
        P("dom", None, None),
        P(("dom", "orb"), None),
    )
    return jax.shard_map(
        body, mesh=mesh, in_specs=placed, out_specs=P(("dom", "orb"), None), check_vma=False
    )
```

```python
import functools

import jax
import jax.numpy as jnp
from jax import lax
from jax.experimental import pallas as pl
from jax.experimental.pallas import tpu as pltpu
from jax.sharding import PartitionSpec as P

SIDE = 48
BUF = 8
DEGREE = 8
SWEEPS = 4
CYCLES = 2
LANES = 128
HALF = 64
SEGMENTS = 4
GROUP = 4
PITCH = 72
SCALE_PITCH = 56


EXCHANGE_FACTOR = (3.0 / 3.141592653589793) ** (1.0 / 3.0)
FOUR_PI = 4.0 * 3.141592653589793
RELAXATION = 0.8
CUTOFF = 1.5


MESH = pl.DeviceIdType.MESH


class Segments:
    def __init__(self, count, box, cells):
        self.count, self.box, self.cells = count, box, cells
        self.lines = cells // SIDE // SEGMENTS
        self.across = LANES // (SEGMENTS * count)
        self.deep = box // self.across
        self.length = self.lines * SIDE
        self.tiles = cells // LANES
        self.blocks = -(-self.length // LANES)
        self.shift = count * self.across
        self.stored = (self.deep + 2) * (self.lines + 2)
        assert self.deep * self.across == box and self.length % HALF == 0
        assert self.tiles * LANES == cells and SIDE % 8 == 0 and box % 8 == 0

    def block(self, plane, line):
        return (plane + 1) * (self.lines + 2) + line + 1

    def spread(self, load, store):
        lane = lax.broadcasted_iota(jnp.int32, (self.across, LANES), 1)
        for plane in range(self.deep):
            kept = {}

            def tile_of(orbital, tile, turned):
                if (orbital, tile, turned) not in kept:
                    value = load(orbital, tile, plane)
                    kept[orbital, tile, turned] = pltpu.roll(value, HALF, 1) if turned else value
                return kept[orbital, tile, turned]

            for block in range(self.blocks):
                rows = min(LANES, self.length - block * LANES)
                pieces = []
                for segment in range(SEGMENTS):
                    first = segment * self.length + block * LANES
                    for orbital in range(self.count):
                        parts = []
                        for half in range(2):
                            cell = min(first + half * HALF, self.cells - HALF)
                            turned = cell % LANES != half * HALF
                            parts.append(tile_of(orbital, cell // LANES, turned))
                        if rows <= HALF or parts[0] is parts[1]:
                            pieces.append(parts[0])
                        else:
                            pieces.append(jnp.where(lane < HALF, parts[0], parts[1]))
                turned = jnp.concatenate(pieces, axis=0).T
                for row in range(0, rows, 8):
                    store(plane, block * LANES + row, turned[row : row + 8])

    def gather(self, load, store):
        lane = lax.broadcasted_iota(jnp.int32, (self.across, LANES), 1)
        for plane in range(self.deep):
            sums = {}
            for block in range(self.blocks):
                rows = min(LANES, self.length - block * LANES)
                pieces = [load(plane, block * LANES + row) for row in range(0, rows, 8)]
                if rows < LANES:
                    pieces.append(jnp.zeros((LANES - rows, LANES), jnp.float32))
                turned = jnp.concatenate(pieces, axis=0).T
                for segment in range(SEGMENTS):
                    base = segment * self.shift
                    value = turned[base : base + self.across]
                    for orbital in range(1, self.count):
                        at = base + orbital * self.across
                        value = value + turned[at : at + self.across]
                    sums[segment, block, False] = value

            def half_of(cell, half):
                segment, place = cell // self.length, cell % self.length
                turned = place % LANES != half * HALF
                key = (segment, place // LANES, turned)
                if key not in sums:
                    sums[key] = pltpu.roll(sums[key[0], key[1], False], HALF, 1)
                return sums[key]

            for tile in range(self.tiles):
                low = half_of(tile * LANES, 0)
                high = half_of(tile * LANES + HALF, 1)
                store(plane, tile, low if low is high else jnp.where(lane < HALF, low, high))


def put_cells(shape, target, plane, start, base, value):
    block = slice(shape.block(plane, start), shape.block(plane, start) + value.shape[0])
    target[block, 8 + base : 16 + base, :] = value
    if base == 0:
        target[block, 8 + SIDE : 9 + SIDE, :] = value[:, :1, :]
    if base == SIDE - 8:
        target[block, 7:8, :] = value[:, 7:, :]


def put_faces(shape, target, plane, start, base, value):
    lines, deep, across = shape.lines, shape.deep, shape.across
    count = value.shape[0]
    cells = slice(8 + base, 16 + base)

    def turn(part, amount):
        return pltpu.roll(part.reshape(-1, LANES), amount, 1).reshape(part.shape)

    def at(plane, line, number):
        first = shape.block(plane, line)
        return slice(first, first + number)

    lane = lax.broadcasted_iota(jnp.int32, value.shape, 2) % across
    if plane == deep - 1:
        target[at(-1, start, count), cells, :] = jnp.where(lane != 0, turn(value, 1), 0.0)
    if plane == 0:
        target[at(deep, start, count), cells, :] = jnp.where(
            lane != across - 1, turn(value, LANES - 1), 0.0
        )
    if start == 0:
        target[at(plane, lines, 1), cells, :] = turn(value[:1], LANES - shape.shift)
    if start + count == lines:
        target[at(plane, -1, 1), cells, :] = turn(value[count - 1 :], shape.shift)


def filter_step(shape, source, target, scale, inverse, first):
    lines, deep = shape.lines, shape.deep
    for base in range(0, SIDE, 8):
        cells = slice(8 + base, 16 + base)
        for start in range(0, lines, GROUP):
            grown = [
                source[shape.block(plane, start - 1) : shape.block(plane, start + GROUP + 1), cells, :]
                if 0 <= plane < deep
                else source[shape.block(plane, start) : shape.block(plane, start + GROUP), cells, :]
                for plane in range(-1, deep + 1)
            ]
            middles = [part[1:-1] if 0 < i <= deep else part for i, part in enumerate(grown)]
            for plane in range(deep):
                first_block = shape.block(plane, start)
                block = slice(first_block, first_block + GROUP)
                rows = slice(plane * lines + start, plane * lines + start + GROUP)
                middle = middles[plane + 1]
                near = source[block, 7 + base : 15 + base, :] + source[block, 9 + base : 17 + base, :]
                near = near + (grown[plane + 1][:-2] + grown[plane + 1][2:])
                near = near + (middles[plane] + middles[plane + 2])
                value = scale[rows, base : base + 8, :] * middle - inverse * near
                if first:
                    value = 0.5 * value
                else:
                    value = value - target[block, cells, :]
                put_cells(shape, target, plane, start, base, value)
                put_faces(shape, target, plane, start, base, value)


def cycles_kernel(doms, ranks, *refs):
    (
        orbitals_hbm, occupations, occupied, weights, ionic_hbm, core_hbm, hartree_hbm,
        output,
        planes_of, ionic, core, flat, weight_rows, even, odd, scale, charge,
        weighted, rim_in, parts, near_h, near_d, work, relaxed, grown, local, box_pot, sums, dom_sums,
        load_sem, rim_send, rim_recv, part_send, part_recv, h_send, h_recv, d_send, d_recv,
        sum_send, sum_recv, dom_send, dom_recv, box_send, box_recv, relay_send,
    ) = refs
    count, box, cells = orbitals_hbm.shape
    chunks, planes, _ = weighted.shape
    shape = Segments(count, box, cells)
    tiles = shape.tiles
    rim = BUF // planes
    span = near_h.shape[1]
    reach = span // 2
    assert planes + 2 * (SWEEPS - 2) <= 8
    everyone = doms * ranks
    dom = lax.axis_index("dom")
    rank = lax.axis_index("orb")
    me = dom * ranks + rank

    def place(index):
        return (lax.div(index, ranks), lax.rem(index, ranks))

    def send(source, target, send_sem, recv_sem, to):
        return pltpu.make_async_remote_copy(
            src_ref=source, dst_ref=target, send_sem=send_sem, recv_sem=recv_sem,
            device_id=to, device_id_type=MESH,
        )

    def repeat(low, high, step):
        lax.fori_loop(low, high, lambda i, carry: (step(i), carry)[1], 0)

    def outward(low, high, step):
        def both(i):
            pl.when(ranks - 1 - i > rank)(lambda: step(ranks - 1 - i))
            pl.when(i < rank)(lambda: step(i))

        repeat(low, high, both)

    def arrived(target, sem):
        send(target, target, sem, sem, (dom, rank)).wait_recv()

    def left(source, sem):
        send(source, source, sem, sem, (dom, rank)).wait_send()

    def loads(source, target, sem):
        for tile in range(tiles):
            pltpu.make_async_copy(
                source.at[:, tile * LANES : (tile + 1) * LANES],
                target.at[tile],
                sem,
            ).start()

    def loaded(target, sem):
        pltpu.make_async_copy(target, target, sem).wait()

    loads(ionic_hbm, ionic, load_sem.at[0])
    for orbital in range(count):
        loads(orbitals_hbm.at[orbital], planes_of.at[orbital], load_sem.at[1])
    guess = pltpu.make_async_copy(hartree_hbm, near_h.at[0, reach], load_sem.at[2])
    guess.start()
    loads(core_hbm, core, load_sem.at[3])

    barrier = pltpu.get_barrier_semaphore()

    def greet(k):
        pl.semaphore_signal(
            barrier, inc=1, device_id=place(lax.rem(me + k, everyone)), device_id_type=MESH
        )

    repeat(1, everyone, greet)

    sublane = lax.broadcasted_iota(jnp.int32, (8, LANES), 0)
    for group in range(0, box, 8):
        rows = jnp.full((8, LANES), weights[0, group], jnp.float32)
        for row in range(1, 8):
            rows = jnp.where(sublane == row, weights[0, group + row], rows)
        weight_rows[group : group + 8, :] = rows

    lane = lax.broadcasted_iota(jnp.int32, (8, LANES), 1)
    orbital_of = lax.rem(lax.div(lane, shape.across), count)

    def strided(ref, tile, plane):
        return ref[tile, pl.ds(plane, shape.across, stride=shape.deep), :]

    def store_orbitals(plane, cell, value):
        put_cells(shape, even, plane, cell // SIDE, cell % SIDE, value[None])

    def store_scale(plane, cell, value):
        scale[plane * shape.lines + cell // SIDE, cell % SIDE : cell % SIDE + 8, :] = value

    def near_copies(cycle, buffer, send_sems, recv_sems):
        copies = []
        for k in range(1, reach + 1):
            for sign in (1, -1):
                to = place(lax.rem(me + sign * k + everyone, everyone))
                slot = reach - sign * k
                copies.append(
                    send(
                        buffer.at[cycle, reach], buffer.at[cycle, slot],
                        send_sems.at[cycle], recv_sems.at[cycle], to,
                    )
                )
        return copies

    factors = []
    for orbital in range(count):
        taken = rank * count + orbital < occupied[0, 0]
        factors.append(
            jnp.where(taken, occupations[0, orbital], jnp.float32(0.0)) / (ranks * count)
        )
    norms = [jnp.float32(1.0)] * count
    height = work.shape[0]
    origin = reach * planes - 2

    def put(target, slot, value):
        run = min(planes, 2)
        for row in range(0, planes, run):
            at = (slot * planes + row - origin) % height
            target[at : at + run, :] = value[row : row + run]

    def relax(field, added):
        for sweep in range(SWEEPS):
            if field is None:
                field = added
                continue
            near = pltpu.roll(field, 1, 0) + pltpu.roll(field, field.shape[0] - 1, 0)
            if sweep == 1:
                field, near = field[:8], near[:8]
            column = lax.broadcasted_iota(jnp.int32, field.shape, 1) % SIDE
            left = jnp.where(
                column == 0, pltpu.roll(field, cells - (SIDE - 1), 1), pltpu.roll(field, 1, 1)
            )
            right = jnp.where(
                column == SIDE - 1, pltpu.roll(field, SIDE - 1, 1),
                pltpu.roll(field, cells - 1, 1),
            )
            near = near + left + right
            near = near + pltpu.roll(field, SIDE, 1) + pltpu.roll(field, cells - SIDE, 1)
            field = field + RELAXATION * (near * (1.0 / 6.0) - field)
            if added is not None:
                field = field + added[: field.shape[0]]
        return field

    work[...] = jnp.zeros_like(work)
    h_copies = None

    for cycle in range(CYCLES):
        last = cycle + 1 == CYCLES
        if cycle == 0:
            loaded(ionic, load_sem.at[0])
            flat[...] = ionic[...]
        else:
            for tile in range(tiles):
                lanes = slice(tile * LANES, (tile + 1) * LANES)
                for group in range(0, box, 8):
                    first = group // planes
                    pieces = [box_pot[first + i, :, lanes] for i in range(8 // planes)]
                    flat[tile, group : group + 8, :] = ionic[
                        tile, group : group + 8, :
                    ] + jnp.concatenate(pieces, axis=0)
        potential = flat[...]
        lowest = jnp.min(jnp.min(potential, axis=0), axis=0, keepdims=True)
        lowest = jnp.min(lowest, axis=1, keepdims=True)
        highest = jnp.max(jnp.max(potential, axis=0), axis=0, keepdims=True)
        highest = jnp.max(highest, axis=1, keepdims=True)
        low_bound = lowest + CUTOFF
        high_bound = highest + 6.0
        center = 0.5 * (high_bound + low_bound)
        inverse = 1.0 / (0.5 * (high_bound - low_bound))
        flat[...] = (2.0 * inverse) * ((3.0 - center) + potential)
        shape.spread(lambda _, tile, plane: strided(flat, tile, plane), store_scale)
        if cycle == 0:
            loaded(planes_of, load_sem.at[1])
            shape.spread(
                lambda orbital, tile, plane: strided(planes_of.at[orbital], tile, plane),
                store_orbitals,
            )
            for base in range(0, SIDE, 8):
                for start in range(0, shape.lines, GROUP):
                    for plane in range(shape.deep):
                        first = shape.block(plane, start)
                        value = even[first : first + GROUP, 8 + base : 16 + base, :]
                        put_faces(shape, even, plane, start, base, value)

        filter_step(shape, even, odd, scale, inverse, True)
        if cycle == 0:
            pl.semaphore_wait(barrier, everyone - 1)
            guess.wait()
        for copy in near_copies(cycle, near_h, h_send, h_recv):
            copy.start()

        def two_steps(step, carry):
            filter_step(shape, odd, even, scale, inverse, False)
            filter_step(shape, even, odd, scale, inverse, False)
            return carry

        lax.fori_loop(0, (DEGREE - 1) // 2, two_steps, 0)
        filter_step(shape, odd, even, scale, inverse, False)

        total = jnp.zeros((8, LANES), jnp.float32)
        for base in range(0, SIDE, 8):
            for plane in range(shape.deep):
                value = even[
                    shape.block(plane, 0) : shape.block(plane, shape.lines), 8 + base : 16 + base, :
                ]
                total = total + jnp.sum(value * value, axis=0)
        shares = jnp.zeros((8, LANES), jnp.float32)
        for orbital in range(count):
            square = jnp.sum(
                jnp.where(orbital_of == orbital, total, 0.0), axis=0, keepdims=True
            )
            square = jnp.sum(square, axis=1, keepdims=True)
            square = norms[orbital] * square * (1.0 / (box * cells)) + 1e-06
            share = factors[orbital] * norms[orbital] / square
            shares = jnp.where(orbital_of == orbital, share, shares)
            norms[orbital] = norms[orbital] / square

        def load_density(plane, cell):
            at = cell % SIDE
            value = even[shape.block(plane, cell // SIDE), 8 + at : 16 + at, :]
            return shares * (value * value)

        def store_density(plane, tile, value):
            flat[tile, pl.ds(plane, shape.across, stride=shape.deep), :] = value

        shape.gather(load_density, store_density)
        if cycle == 0:
            loaded(core, load_sem.at[3])
        def weigh(groups, found):
            for group in groups:
                rows = slice(group, group + 8)
                weight = weight_rows[rows, :]
                for tile in range(tiles):
                    density = flat[tile, rows, :] + core[tile, rows, :] * (1.0 / ranks)
                    density = density * weight
                    found = found + density
                    for piece in range(8 // planes):
                        weighted[
                            group // planes + piece, :, tile * LANES : (tile + 1) * LANES
                        ] = density[piece * planes : (piece + 1) * planes]
            return found

        outer = list(range(0, BUF, 8)) + list(range(box - BUF, box, 8))
        edges = list(range(BUF, 2 * BUF, 8)) + list(range(box - 2 * BUF, box - BUF, 8))
        found = jnp.zeros((8, LANES), jnp.float32) if cycle == 0 else charge[...]
        found = weigh(outer, found)
        down = (lax.rem(dom + doms - 1, doms), rank)
        up = (lax.rem(dom + 1, doms), rank)
        rims = [
            send(
                weighted.at[:rim], rim_in.at[cycle, 1],
                rim_send.at[cycle], rim_recv.at[cycle, 1], down,
            ),
            send(
                weighted.at[rim + ranks :], rim_in.at[cycle, 0],
                rim_send.at[cycle], rim_recv.at[cycle, 0], up,
            ),
        ]
        for copy in rims:
            copy.start()
        found = weigh([g for g in range(2 * BUF, box - 2 * BUF, 8)], found)

        def sum_copy(k):
            to = (dom, lax.rem(rank + k, ranks))
            return send(sums.at[rank], sums.at[rank], sum_send.at[0], sum_recv.at[0], to)

        def part_copy(owner, cycle=cycle):
            return send(
                weighted.at[owner + rim], parts.at[cycle, rank],
                part_send.at[cycle], part_recv.at[cycle], (dom, owner),
            )

        def give(owner):
            part_copy(owner).start()

        def delayed(owner):
            apart = (2 * owner >= ranks) != (2 * rank >= ranks)
            return jnp.logical_and(apart, lax.rem(owner + rank, 2) == 1)

        def give_now(owner):
            pl.when(jnp.logical_not(delayed(owner)))(lambda: give(owner))

        def give_later(owner):
            pl.when(delayed(owner))(lambda: give(owner))

        outward(rim, ranks - rim, give_now)
        found = weigh(edges, found)
        if last:
            sums[rank] = found
            repeat(1, ranks, lambda k: sum_copy(k).start())
        else:
            charge[...] = found

        def join(step):
            side = lax.rem(dom + 1 + step, 2)
            arrived(rim_in.at[cycle, side], rim_recv.at[cycle, side])
            base = side * (ranks - rim)
            for j in range(rim):
                weighted[rim + base + j] += rim_in[cycle, side, j]
                pl.when(base + j != rank)(lambda: give(base + j))

        repeat(0, 2, join)
        outward(rim, ranks - rim, give_later)

        arrived(near_h.at[cycle, : span - 1], h_recv.at[cycle])
        for slot in range(span):
            put(work, slot, near_h[cycle, slot])
        relaxed[...] = relax(work[...], None)

        def dom_copy(k):
            to = (lax.rem(dom + k, doms), rank)
            return send(dom_sums.at[dom], dom_sums.at[dom], dom_send.at[0], dom_recv.at[0], to)

        arrived(parts.at[cycle, : ranks - 1], part_recv.at[cycle])
        density = weighted[rank + rim]
        for k in range(1, ranks):
            density = density + parts[cycle, lax.rem(rank + k, ranks)]
        near_d[cycle, reach] = density
        d_copies = near_copies(cycle, near_d, d_send, d_recv)
        for copy in d_copies:
            copy.start()

        if last:
            arrived(sums.at[: ranks - 1], sum_recv.at[0])
            dom_sums[dom] = jnp.sum(sums[...], axis=0)
            repeat(1, doms, lambda k: dom_copy(k).start())

        root = jnp.exp(jnp.log(density) * (1.0 / 3.0))
        root = root - (root - density / (root * root)) * (1.0 / 3.0)
        local[...] = relaxed[2 : 2 + planes, :] - EXCHANGE_FACTOR * root
        arrived(near_d.at[cycle, : span - 1], d_recv.at[cycle])
        for slot in range(span):
            put(work, slot, near_d[cycle, slot])
        if last:
            arrived(dom_sums.at[: doms - 1], dom_recv.at[0])
            total = jnp.sum(jnp.sum(dom_sums[...], axis=0), axis=0, keepdims=True)
            total = jnp.sum(total, axis=1, keepdims=True)
            average = total / (everyone * planes * cells)
            shift = (-SWEEPS * RELAXATION * FOUR_PI / 6.0) * average
            local[...] += shift
        change = relax(None, (RELAXATION * FOUR_PI / 6.0) * work[...])
        grown[...] = change
        change = grown[2 : 2 + planes, :]
        result = local[...] + change

        left(near_h.at[cycle, : span - 1], h_send.at[cycle])
        if not last:
            slot = rank + rim
            box_pot[slot] = result

            late = jnp.where(rank >= ranks - rim, rank - (ranks - 2 * rim), 2 * rim)
            box_sem = jnp.where(rank < rim, rank, late)

            def box_copy(to):
                return send(
                    box_pot.at[rank + rim], box_pot.at[rank + rim],
                    box_send.at[0], box_recv.at[box_sem], (dom, to),
                )

            outward(0, ranks, lambda to: box_copy(to).start())
            near_h[cycle + 1, reach] = relaxed[2 : 2 + planes, :] + change

            def relay_copy(index):
                side, j = lax.div(index, rim), lax.rem(index, rim)
                owner = side * (ranks - rim) + j
                target = jnp.where(side == 0, chunks - rim + j, j)
                to_dom = lax.rem(dom + jnp.where(side == 0, doms - 1, 1), doms)
                return send(
                    box_pot.at[owner + rim], box_pot.at[target],
                    relay_send.at[0], box_recv.at[2 * rim], (to_dom, rank),
                )

            def relay(step):
                index = lax.rem(step + rim * lax.rem(dom + 1, 2), 2 * rim)
                side, j = lax.div(index, rim), lax.rem(index, rim)
                owner = side * (ranks - rim) + j

                @pl.when(owner != rank)
                def _():
                    arrived(box_pot.at[owner + rim], box_recv.at[index])

                relay_copy(index).start()

            repeat(0, 2 * rim, relay)
            at_edge = box_sem < 2 * rim

            @pl.when(at_edge)
            def _():
                arrived(box_pot.at[:ranks], box_recv.at[2 * rim])

            @pl.when(jnp.logical_not(at_edge))
            def _():
                arrived(box_pot.at[: ranks - 1], box_recv.at[2 * rim])

            left(box_pot.at[: ranks - 1], box_send.at[0])
            left(box_pot.at[: 2 * rim], relay_send.at[0])

        left(rim_in.at[cycle], rim_send.at[cycle])
        left(near_d.at[cycle, : span - 1], d_send.at[cycle])
        left(parts.at[cycle, : ranks - 1], part_send.at[cycle])
        if last:
            output[...] = result
            left(sums.at[: ranks - 1], sum_send.at[0])
            left(dom_sums.at[: doms - 1], dom_send.at[0])


def body(
    orbitals, occupations, occupied_count, weights, external_potential, core_density, hartree_guess
):
    doms, ranks = lax.axis_size("dom"), lax.axis_size("orb")
    count, box, cells = orbitals.shape[1:]
    planes = hartree_guess.shape[0]
    chunks = box // planes
    rim = BUF // planes
    reach = -(-SWEEPS // planes)
    span = 2 * reach + 1
    rows = -(-span * planes // 8) * 8
    shape = Segments(count, box, cells)
    lines = shape.deep * shape.lines
    f32 = jnp.float32
    anywhere = pl.BlockSpec(memory_space=pl.ANY)
    scalars = pl.BlockSpec(memory_space=pltpu.SMEM)
    dma = pltpu.SemaphoreType.DMA
    vmem = lambda *dims: pltpu.VMEM(dims, f32)
    return pl.pallas_call(
        functools.partial(cycles_kernel, doms, ranks),
        out_shape=pltpu.VMEM((planes, cells), f32),
        in_specs=[anywhere, scalars, scalars, scalars, anywhere, anywhere, anywhere],
        out_specs=pl.BlockSpec(memory_space=pltpu.VMEM),
        scratch_shapes=[
            vmem(count, shape.tiles, box, LANES),
            vmem(shape.tiles, box, LANES),
            vmem(shape.tiles, box, LANES),
            vmem(shape.tiles, box, LANES),
            vmem(box, LANES),
            vmem(shape.stored, PITCH, LANES),
            vmem(shape.stored, PITCH, LANES),
            vmem(lines, SCALE_PITCH, LANES),
            vmem(8, LANES),
            vmem(chunks, planes, cells),
            vmem(CYCLES, 2, rim, planes, cells),
            vmem(CYCLES, ranks, planes, cells),
            vmem(CYCLES, span, planes, cells),
            vmem(CYCLES, span, planes, cells),
            vmem(rows, cells),
            vmem(8, cells),
            vmem(8, cells),
            vmem(planes, cells),
            vmem(chunks, planes, cells),
            vmem(ranks, 8, LANES),
            vmem(doms, 8, LANES),
            dma((4,)),
            dma((CYCLES,)), dma((CYCLES, 2)),
            dma((CYCLES,)), dma((CYCLES,)),
            dma((CYCLES,)), dma((CYCLES,)),
            dma((CYCLES,)), dma((CYCLES,)),
            dma((1,)), dma((1,)),
            dma((1,)), dma((1,)),
            dma((1,)), dma((2 * rim + 1,)),
            dma((1,)),
        ],
        compiler_params=pltpu.CompilerParams(collective_id=0, has_side_effects=True),
        name="cycles",
    )(
        orbitals[0], occupations, occupied_count.reshape(1, 1), weights, external_potential[0],
        core_density[0], hartree_guess,
    )


def solution(mesh):
    placed = (
        P("dom", "orb", None, None),
        P("dom", "orb"),
        P("dom"),
        P("dom", None),
        P("dom", None, None),
        P("dom", None, None),
        P(("dom", "orb"), None),
    )
    return jax.shard_map(
        body, mesh=mesh, in_specs=placed, out_specs=P(("dom", "orb"), None), check_vma=False
    )
```

```python
import functools

import jax
import jax.numpy as jnp
from jax import lax
from jax.experimental import pallas as pl
from jax.experimental.pallas import tpu as pltpu
from jax.sharding import PartitionSpec as P

SIDE = 48
BUF = 8
DEGREE = 8
SWEEPS = 4
CYCLES = 2
LANES = 128
HALF = 64
SEGMENTS = 4
GROUP = 4
PITCH = 72
SCALE_PITCH = 56


EXCHANGE_FACTOR = (3.0 / 3.141592653589793) ** (1.0 / 3.0)
FOUR_PI = 4.0 * 3.141592653589793
RELAXATION = 0.8
CUTOFF = 1.5


MESH = pl.DeviceIdType.MESH


class Segments:
    def __init__(self, count, box, cells):
        self.count, self.box, self.cells = count, box, cells
        self.lines = cells // SIDE // SEGMENTS
        self.across = LANES // (SEGMENTS * count)
        self.deep = box // self.across
        self.length = self.lines * SIDE
        self.tiles = cells // LANES
        self.blocks = -(-self.length // LANES)
        self.shift = count * self.across
        self.stored = (self.deep + 2) * (self.lines + 2)
        assert self.deep * self.across == box and self.length % HALF == 0
        assert self.tiles * LANES == cells and SIDE % 8 == 0 and box % 8 == 0

    def block(self, plane, line):
        return (plane + 1) * (self.lines + 2) + line + 1

    def spread(self, load, store):
        lane = lax.broadcasted_iota(jnp.int32, (self.across, LANES), 1)
        for plane in range(self.deep):
            kept = {}

            def tile_of(orbital, tile, turned):
                if (orbital, tile, turned) not in kept:
                    value = load(orbital, tile, plane)
                    kept[orbital, tile, turned] = pltpu.roll(value, HALF, 1) if turned else value
                return kept[orbital, tile, turned]

            for block in range(self.blocks):
                rows = min(LANES, self.length - block * LANES)
                pieces = []
                for segment in range(SEGMENTS):
                    first = segment * self.length + block * LANES
                    for orbital in range(self.count):
                        parts = []
                        for half in range(2):
                            cell = min(first + half * HALF, self.cells - HALF)
                            turned = cell % LANES != half * HALF
                            parts.append(tile_of(orbital, cell // LANES, turned))
                        if rows <= HALF or parts[0] is parts[1]:
                            pieces.append(parts[0])
                        else:
                            pieces.append(jnp.where(lane < HALF, parts[0], parts[1]))
                turned = jnp.concatenate(pieces, axis=0).T
                for row in range(0, rows, 8):
                    store(plane, block * LANES + row, turned[row : row + 8])

    def gather(self, load, store):
        lane = lax.broadcasted_iota(jnp.int32, (self.across, LANES), 1)
        for plane in range(self.deep):
            sums = {}
            for block in range(self.blocks):
                rows = min(LANES, self.length - block * LANES)
                pieces = [load(plane, block * LANES + row) for row in range(0, rows, 8)]
                if rows < LANES:
                    pieces.append(jnp.zeros((LANES - rows, LANES), jnp.float32))
                turned = jnp.concatenate(pieces, axis=0).T
                for segment in range(SEGMENTS):
                    base = segment * self.shift
                    value = turned[base : base + self.across]
                    for orbital in range(1, self.count):
                        at = base + orbital * self.across
                        value = value + turned[at : at + self.across]
                    sums[segment, block, False] = value

            def half_of(cell, half):
                segment, place = cell // self.length, cell % self.length
                turned = place % LANES != half * HALF
                key = (segment, place // LANES, turned)
                if key not in sums:
                    sums[key] = pltpu.roll(sums[key[0], key[1], False], HALF, 1)
                return sums[key]

            for tile in range(self.tiles):
                low = half_of(tile * LANES, 0)
                high = half_of(tile * LANES + HALF, 1)
                store(plane, tile, low if low is high else jnp.where(lane < HALF, low, high))


def put_cells(shape, target, plane, start, base, value):
    block = slice(shape.block(plane, start), shape.block(plane, start) + value.shape[0])
    target[block, 8 + base : 16 + base, :] = value
    if base == 0:
        target[block, 8 + SIDE : 9 + SIDE, :] = value[:, :1, :]
    if base == SIDE - 8:
        target[block, 7:8, :] = value[:, 7:, :]


def put_faces(shape, target, plane, start, base, value):
    lines, deep, across = shape.lines, shape.deep, shape.across
    count = value.shape[0]
    cells = slice(8 + base, 16 + base)

    def turn(part, amount):
        return pltpu.roll(part.reshape(-1, LANES), amount, 1).reshape(part.shape)

    def at(plane, line, number):
        first = shape.block(plane, line)
        return slice(first, first + number)

    lane = lax.broadcasted_iota(jnp.int32, value.shape, 2) % across
    if plane == deep - 1:
        target[at(-1, start, count), cells, :] = jnp.where(lane != 0, turn(value, 1), 0.0)
    if plane == 0:
        target[at(deep, start, count), cells, :] = jnp.where(
            lane != across - 1, turn(value, LANES - 1), 0.0
        )
    if start == 0:
        target[at(plane, lines, 1), cells, :] = turn(value[:1], LANES - shape.shift)
    if start + count == lines:
        target[at(plane, -1, 1), cells, :] = turn(value[count - 1 :], shape.shift)


def filter_step(shape, source, target, scale, inverse, first):
    lines, deep = shape.lines, shape.deep
    for base in range(0, SIDE, 8):
        cells = slice(8 + base, 16 + base)
        for start in range(0, lines, GROUP):
            grown = [
                source[shape.block(plane, start - 1) : shape.block(plane, start + GROUP + 1), cells, :]
                if 0 <= plane < deep
                else source[shape.block(plane, start) : shape.block(plane, start + GROUP), cells, :]
                for plane in range(-1, deep + 1)
            ]
            middles = [part[1:-1] if 0 < i <= deep else part for i, part in enumerate(grown)]
            for plane in range(deep):
                first_block = shape.block(plane, start)
                block = slice(first_block, first_block + GROUP)
                rows = slice(plane * lines + start, plane * lines + start + GROUP)
                middle = middles[plane + 1]
                near = source[block, 7 + base : 15 + base, :] + source[block, 9 + base : 17 + base, :]
                near = near + (grown[plane + 1][:-2] + grown[plane + 1][2:])
                near = near + (middles[plane] + middles[plane + 2])
                value = scale[rows, base : base + 8, :] * middle - inverse * near
                if first:
                    value = 0.5 * value
                else:
                    value = value - target[block, cells, :]
                put_cells(shape, target, plane, start, base, value)
                put_faces(shape, target, plane, start, base, value)


def cycles_kernel(doms, ranks, *refs):
    (
        orbitals_hbm, occupations, occupied, weights, ionic_hbm, core_hbm, hartree_hbm,
        output,
        planes_of, ionic, core, flat, weight_rows, even, odd, scale, charge,
        weighted, rim_in, parts, near_h, near_d, work, relaxed, grown, local, box_pot, sums, dom_sums,
        load_sem, rim_send, rim_recv, part_send, part_recv, h_send, h_recv, d_send, d_recv,
        sum_send, sum_recv, dom_send, dom_recv, box_send, box_recv, relay_send,
    ) = refs
    count, box, cells = orbitals_hbm.shape
    chunks, planes, _ = weighted.shape
    shape = Segments(count, box, cells)
    tiles = shape.tiles
    rim = BUF // planes
    span = near_h.shape[1]
    reach = span // 2
    assert planes + 2 * (SWEEPS - 2) <= 8
    everyone = doms * ranks
    dom = lax.axis_index("dom")
    rank = lax.axis_index("orb")
    me = dom * ranks + rank

    def place(index):
        return (lax.div(index, ranks), lax.rem(index, ranks))

    def send(source, target, send_sem, recv_sem, to):
        return pltpu.make_async_remote_copy(
            src_ref=source, dst_ref=target, send_sem=send_sem, recv_sem=recv_sem,
            device_id=to, device_id_type=MESH,
        )

    def repeat(low, high, step):
        lax.fori_loop(low, high, lambda i, carry: (step(i), carry)[1], 0)

    def outward(low, high, step):
        def both(i):
            pl.when(ranks - 1 - i > rank)(lambda: step(ranks - 1 - i))
            pl.when(i < rank)(lambda: step(i))

        repeat(low, high, both)

    def arrived(target, sem):
        send(target, target, sem, sem, (dom, rank)).wait_recv()

    def left(source, sem):
        send(source, source, sem, sem, (dom, rank)).wait_send()

    def loads(source, target, sem):
        for tile in range(tiles):
            pltpu.make_async_copy(
                source.at[:, tile * LANES : (tile + 1) * LANES],
                target.at[tile],
                sem,
            ).start()

    def loaded(target, sem):
        pltpu.make_async_copy(target, target, sem).wait()

    loads(ionic_hbm, ionic, load_sem.at[0])
    for orbital in range(count):
        loads(orbitals_hbm.at[orbital], planes_of.at[orbital], load_sem.at[1])
    guess = pltpu.make_async_copy(hartree_hbm, near_h.at[0, reach], load_sem.at[2])
    guess.start()
    loads(core_hbm, core, load_sem.at[3])

    barrier = pltpu.get_barrier_semaphore()

    def greet(to):
        pl.semaphore_signal(barrier, inc=1, device_id=to, device_id_type=MESH)

    repeat(1, ranks, lambda k: greet((dom, lax.rem(rank + k, ranks))))
    repeat(1, doms, lambda k: greet((lax.rem(dom + k, doms), rank)))
    for k in range(1, reach + 1):
        greet(place(lax.rem(me + k, everyone)))
        greet(place(lax.rem(me - k + everyone, everyone)))

    sublane = lax.broadcasted_iota(jnp.int32, (8, LANES), 0)
    for group in range(0, box, 8):
        rows = jnp.full((8, LANES), weights[0, group], jnp.float32)
        for row in range(1, 8):
            rows = jnp.where(sublane == row, weights[0, group + row], rows)
        weight_rows[group : group + 8, :] = rows

    lane = lax.broadcasted_iota(jnp.int32, (8, LANES), 1)
    orbital_of = lax.rem(lax.div(lane, shape.across), count)

    def strided(ref, tile, plane):
        return ref[tile, pl.ds(plane, shape.across, stride=shape.deep), :]

    def store_orbitals(plane, cell, value):
        put_cells(shape, even, plane, cell // SIDE, cell % SIDE, value[None])

    def store_scale(plane, cell, value):
        scale[plane * shape.lines + cell // SIDE, cell % SIDE : cell % SIDE + 8, :] = value

    def near_copies(cycle, buffer, send_sems, recv_sems):
        copies = []
        for k in range(1, reach + 1):
            for sign in (1, -1):
                to = place(lax.rem(me + sign * k + everyone, everyone))
                slot = reach - sign * k
                copies.append(
                    send(
                        buffer.at[cycle, reach], buffer.at[cycle, slot],
                        send_sems.at[cycle], recv_sems.at[cycle], to,
                    )
                )
        return copies

    factors = []
    for orbital in range(count):
        taken = rank * count + orbital < occupied[0, 0]
        factors.append(
            jnp.where(taken, occupations[0, orbital], jnp.float32(0.0)) / (ranks * count)
        )
    norms = [jnp.float32(1.0)] * count
    height = work.shape[0]
    origin = reach * planes - 2

    def put(target, slot, value):
        run = min(planes, 2)
        for row in range(0, planes, run):
            at = (slot * planes + row - origin) % height
            target[at : at + run, :] = value[row : row + run]

    def relax(field, added):
        for sweep in range(SWEEPS):
            if field is None:
                field = added
                continue
            near = pltpu.roll(field, 1, 0) + pltpu.roll(field, field.shape[0] - 1, 0)
            if sweep == 1:
                field, near = field[:8], near[:8]
            column = lax.broadcasted_iota(jnp.int32, field.shape, 1) % SIDE
            left = jnp.where(
                column == 0, pltpu.roll(field, cells - (SIDE - 1), 1), pltpu.roll(field, 1, 1)
            )
            right = jnp.where(
                column == SIDE - 1, pltpu.roll(field, SIDE - 1, 1),
                pltpu.roll(field, cells - 1, 1),
            )
            near = near + left + right
            near = near + pltpu.roll(field, SIDE, 1) + pltpu.roll(field, cells - SIDE, 1)
            field = field + RELAXATION * (near * (1.0 / 6.0) - field)
            if added is not None:
                field = field + added[: field.shape[0]]
        return field

    work[...] = jnp.zeros_like(work)
    h_copies = None

    for cycle in range(CYCLES):
        last = cycle + 1 == CYCLES
        if cycle == 0:
            loaded(ionic, load_sem.at[0])
            flat[...] = ionic[...]
        else:
            for tile in range(tiles):
                lanes = slice(tile * LANES, (tile + 1) * LANES)
                for group in range(0, box, 8):
                    first = group // planes
                    pieces = [box_pot[first + i, :, lanes] for i in range(8 // planes)]
                    flat[tile, group : group + 8, :] = ionic[
                        tile, group : group + 8, :
                    ] + jnp.concatenate(pieces, axis=0)
        potential = flat[...]
        lowest = jnp.min(jnp.min(potential, axis=0), axis=0, keepdims=True)
        lowest = jnp.min(lowest, axis=1, keepdims=True)
        highest = jnp.max(jnp.max(potential, axis=0), axis=0, keepdims=True)
        highest = jnp.max(highest, axis=1, keepdims=True)
        low_bound = lowest + CUTOFF
        high_bound = highest + 6.0
        center = 0.5 * (high_bound + low_bound)
        inverse = 1.0 / (0.5 * (high_bound - low_bound))
        flat[...] = (2.0 * inverse) * ((3.0 - center) + potential)
        shape.spread(lambda _, tile, plane: strided(flat, tile, plane), store_scale)
        if cycle == 0:
            loaded(planes_of, load_sem.at[1])
            shape.spread(
                lambda orbital, tile, plane: strided(planes_of.at[orbital], tile, plane),
                store_orbitals,
            )
            for base in range(0, SIDE, 8):
                for start in range(0, shape.lines, GROUP):
                    for plane in range(shape.deep):
                        first = shape.block(plane, start)
                        value = even[first : first + GROUP, 8 + base : 16 + base, :]
                        put_faces(shape, even, plane, start, base, value)

        filter_step(shape, even, odd, scale, inverse, True)
        if cycle == 0:
            pl.semaphore_wait(barrier, ranks + doms - 2 + 2 * reach)
            guess.wait()
        for copy in near_copies(cycle, near_h, h_send, h_recv):
            copy.start()

        def two_steps(step, carry):
            filter_step(shape, odd, even, scale, inverse, False)
            filter_step(shape, even, odd, scale, inverse, False)
            return carry

        lax.fori_loop(0, (DEGREE - 1) // 2, two_steps, 0)
        filter_step(shape, odd, even, scale, inverse, False)

        total = jnp.zeros((8, LANES), jnp.float32)
        for base in range(0, SIDE, 8):
            for plane in range(shape.deep):
                value = even[
                    shape.block(plane, 0) : shape.block(plane, shape.lines), 8 + base : 16 + base, :
                ]
                total = total + jnp.sum(value * value, axis=0)
        shares = jnp.zeros((8, LANES), jnp.float32)
        for orbital in range(count):
            square = jnp.sum(
                jnp.where(orbital_of == orbital, total, 0.0), axis=0, keepdims=True
            )
            square = jnp.sum(square, axis=1, keepdims=True)
            square = norms[orbital] * square * (1.0 / (box * cells)) + 1e-06
            share = factors[orbital] * norms[orbital] / square
            shares = jnp.where(orbital_of == orbital, share, shares)
            norms[orbital] = norms[orbital] / square

        def load_density(plane, cell):
            at = cell % SIDE
            value = even[shape.block(plane, cell // SIDE), 8 + at : 16 + at, :]
            return shares * (value * value)

        def store_density(plane, tile, value):
            flat[tile, pl.ds(plane, shape.across, stride=shape.deep), :] = value

        shape.gather(load_density, store_density)
        if cycle == 0:
            loaded(core, load_sem.at[3])
        def weigh(groups, found):
            for group in groups:
                rows = slice(group, group + 8)
                weight = weight_rows[rows, :]
                for tile in range(tiles):
                    density = flat[tile, rows, :] + core[tile, rows, :] * (1.0 / ranks)
                    density = density * weight
                    found = found + density
                    for piece in range(8 // planes):
                        weighted[
                            group // planes + piece, :, tile * LANES : (tile + 1) * LANES
                        ] = density[piece * planes : (piece + 1) * planes]
            return found

        outer = list(range(0, BUF, 8)) + list(range(box - BUF, box, 8))
        edges = list(range(BUF, 2 * BUF, 8)) + list(range(box - 2 * BUF, box - BUF, 8))
        found = jnp.zeros((8, LANES), jnp.float32) if cycle == 0 else charge[...]
        found = weigh(outer, found)
        down = (lax.rem(dom + doms - 1, doms), rank)
        up = (lax.rem(dom + 1, doms), rank)
        rims = [
            send(
                weighted.at[:rim], rim_in.at[cycle, 1],
                rim_send.at[cycle], rim_recv.at[cycle, 1], down,
            ),
            send(
                weighted.at[rim + ranks :], rim_in.at[cycle, 0],
                rim_send.at[cycle], rim_recv.at[cycle, 0], up,
            ),
        ]
        for copy in rims:
            copy.start()
        found = weigh([g for g in range(2 * BUF, box - 2 * BUF, 8)], found)

        def sum_copy(k):
            to = (dom, lax.rem(rank + k, ranks))
            return send(sums.at[rank], sums.at[rank], sum_send.at[0], sum_recv.at[0], to)

        def part_copy(owner, cycle=cycle):
            return send(
                weighted.at[owner + rim], parts.at[cycle, rank],
                part_send.at[cycle], part_recv.at[cycle], (dom, owner),
            )

        def give(owner):
            part_copy(owner).start()

        def delayed(owner):
            apart = (2 * owner >= ranks) != (2 * rank >= ranks)
            return jnp.logical_and(apart, lax.rem(owner + rank, 2) == 1)

        def give_now(owner):
            pl.when(jnp.logical_not(delayed(owner)))(lambda: give(owner))

        def give_later(owner):
            pl.when(delayed(owner))(lambda: give(owner))

        outward(rim, ranks - rim, give_now)
        found = weigh(edges, found)
        if last:
            sums[rank] = found
            repeat(1, ranks, lambda k: sum_copy(k).start())
        else:
            charge[...] = found

        def join(step):
            side = lax.rem(dom + 1 + step, 2)
            arrived(rim_in.at[cycle, side], rim_recv.at[cycle, side])
            base = side * (ranks - rim)
            for j in range(rim):
                weighted[rim + base + j] += rim_in[cycle, side, j]
                pl.when(base + j != rank)(lambda: give(base + j))

        repeat(0, 2, join)
        outward(rim, ranks - rim, give_later)

        arrived(near_h.at[cycle, : span - 1], h_recv.at[cycle])
        for slot in range(span):
            put(work, slot, near_h[cycle, slot])
        relaxed[...] = relax(work[...], None)

        def dom_copy(k):
            to = (lax.rem(dom + k, doms), rank)
            return send(dom_sums.at[dom], dom_sums.at[dom], dom_send.at[0], dom_recv.at[0], to)

        arrived(parts.at[cycle, : ranks - 1], part_recv.at[cycle])
        density = weighted[rank + rim]
        for k in range(1, ranks):
            density = density + parts[cycle, lax.rem(rank + k, ranks)]
        near_d[cycle, reach] = density
        d_copies = near_copies(cycle, near_d, d_send, d_recv)
        for copy in d_copies:
            copy.start()

        if last:
            arrived(sums.at[: ranks - 1], sum_recv.at[0])
            dom_sums[dom] = jnp.sum(sums[...], axis=0)
            repeat(1, doms, lambda k: dom_copy(k).start())

        root = jnp.exp(jnp.log(density) * (1.0 / 3.0))
        root = root - (root - density / (root * root)) * (1.0 / 3.0)
        local[...] = relaxed[2 : 2 + planes, :] - EXCHANGE_FACTOR * root
        arrived(near_d.at[cycle, : span - 1], d_recv.at[cycle])
        for slot in range(span):
            put(work, slot, near_d[cycle, slot])
        if last:
            arrived(dom_sums.at[: doms - 1], dom_recv.at[0])
            total = jnp.sum(jnp.sum(dom_sums[...], axis=0), axis=0, keepdims=True)
            total = jnp.sum(total, axis=1, keepdims=True)
            average = total / (everyone * planes * cells)
            shift = (-SWEEPS * RELAXATION * FOUR_PI / 6.0) * average
            local[...] += shift
        change = relax(None, (RELAXATION * FOUR_PI / 6.0) * work[...])
        grown[...] = change
        change = grown[2 : 2 + planes, :]
        result = local[...] + change

        left(near_h.at[cycle, : span - 1], h_send.at[cycle])
        if not last:
            slot = rank + rim
            box_pot[slot] = result

            late = jnp.where(rank >= ranks - rim, rank - (ranks - 2 * rim), 2 * rim)
            box_sem = jnp.where(rank < rim, rank, late)

            def box_copy(to):
                return send(
                    box_pot.at[rank + rim], box_pot.at[rank + rim],
                    box_send.at[0], box_recv.at[box_sem], (dom, to),
                )

            outward(0, ranks, lambda to: box_copy(to).start())
            near_h[cycle + 1, reach] = relaxed[2 : 2 + planes, :] + change

            def relay_copy(index):
                side, j = lax.div(index, rim), lax.rem(index, rim)
                owner = side * (ranks - rim) + j
                target = jnp.where(side == 0, chunks - rim + j, j)
                to_dom = lax.rem(dom + jnp.where(side == 0, doms - 1, 1), doms)
                return send(
                    box_pot.at[owner + rim], box_pot.at[target],
                    relay_send.at[0], box_recv.at[2 * rim], (to_dom, rank),
                )

            def relay(step):
                index = lax.rem(step + rim * lax.rem(dom + 1, 2), 2 * rim)
                side, j = lax.div(index, rim), lax.rem(index, rim)
                owner = side * (ranks - rim) + j

                @pl.when(owner != rank)
                def _():
                    arrived(box_pot.at[owner + rim], box_recv.at[index])

                relay_copy(index).start()

            repeat(0, 2 * rim, relay)
            at_edge = box_sem < 2 * rim

            @pl.when(at_edge)
            def _():
                arrived(box_pot.at[:ranks], box_recv.at[2 * rim])

            @pl.when(jnp.logical_not(at_edge))
            def _():
                arrived(box_pot.at[: ranks - 1], box_recv.at[2 * rim])

            left(box_pot.at[: ranks - 1], box_send.at[0])
            left(box_pot.at[: 2 * rim], relay_send.at[0])

        left(rim_in.at[cycle], rim_send.at[cycle])
        left(near_d.at[cycle, : span - 1], d_send.at[cycle])
        left(parts.at[cycle, : ranks - 1], part_send.at[cycle])
        if last:
            output[...] = result
            left(sums.at[: ranks - 1], sum_send.at[0])
            left(dom_sums.at[: doms - 1], dom_send.at[0])


def body(
    orbitals, occupations, occupied_count, weights, external_potential, core_density, hartree_guess
):
    doms, ranks = lax.axis_size("dom"), lax.axis_size("orb")
    count, box, cells = orbitals.shape[1:]
    planes = hartree_guess.shape[0]
    chunks = box // planes
    rim = BUF // planes
    reach = -(-SWEEPS // planes)
    span = 2 * reach + 1
    rows = -(-span * planes // 8) * 8
    shape = Segments(count, box, cells)
    lines = shape.deep * shape.lines
    f32 = jnp.float32
    anywhere = pl.BlockSpec(memory_space=pl.ANY)
    scalars = pl.BlockSpec(memory_space=pltpu.SMEM)
    dma = pltpu.SemaphoreType.DMA
    vmem = lambda *dims: pltpu.VMEM(dims, f32)
    return pl.pallas_call(
        functools.partial(cycles_kernel, doms, ranks),
        out_shape=pltpu.VMEM((planes, cells), f32),
        in_specs=[anywhere, scalars, scalars, scalars, anywhere, anywhere, anywhere],
        out_specs=pl.BlockSpec(memory_space=pltpu.VMEM),
        scratch_shapes=[
            vmem(count, shape.tiles, box, LANES),
            vmem(shape.tiles, box, LANES),
            vmem(shape.tiles, box, LANES),
            vmem(shape.tiles, box, LANES),
            vmem(box, LANES),
            vmem(shape.stored, PITCH, LANES),
            vmem(shape.stored, PITCH, LANES),
            vmem(lines, SCALE_PITCH, LANES),
            vmem(8, LANES),
            vmem(chunks, planes, cells),
            vmem(CYCLES, 2, rim, planes, cells),
            vmem(CYCLES, ranks, planes, cells),
            vmem(CYCLES, span, planes, cells),
            vmem(CYCLES, span, planes, cells),
            vmem(rows, cells),
            vmem(8, cells),
            vmem(8, cells),
            vmem(planes, cells),
            vmem(chunks, planes, cells),
            vmem(ranks, 8, LANES),
            vmem(doms, 8, LANES),
            dma((4,)),
            dma((CYCLES,)), dma((CYCLES, 2)),
            dma((CYCLES,)), dma((CYCLES,)),
            dma((CYCLES,)), dma((CYCLES,)),
            dma((CYCLES,)), dma((CYCLES,)),
            dma((1,)), dma((1,)),
            dma((1,)), dma((1,)),
            dma((1,)), dma((2 * rim + 1,)),
            dma((1,)),
        ],
        compiler_params=pltpu.CompilerParams(collective_id=0, has_side_effects=True),
        name="cycles",
    )(
        orbitals[0], occupations, occupied_count.reshape(1, 1), weights, external_potential[0],
        core_density[0], hartree_guess,
    )


def solution(mesh):
    placed = (
        P("dom", "orb", None, None),
        P("dom", "orb"),
        P("dom"),
        P("dom", None),
        P("dom", None, None),
        P("dom", None, None),
        P(("dom", "orb"), None),
    )
    return jax.shard_map(
        body, mesh=mesh, in_specs=placed, out_specs=P(("dom", "orb"), None), check_vma=False
    )
```

```python
import functools

import jax
import jax.numpy as jnp
from jax import lax
from jax.experimental import pallas as pl
from jax.experimental.pallas import tpu as pltpu
from jax.sharding import PartitionSpec as P

SIDE = 48
BUF = 8
DEGREE = 8
SWEEPS = 4
CYCLES = 2
LANES = 128
HALF = 64
SEGMENTS = 4
GROUP = 4
PITCH = 72
SCALE_PITCH = 56


EXCHANGE_FACTOR = (3.0 / 3.141592653589793) ** (1.0 / 3.0)
FOUR_PI = 4.0 * 3.141592653589793
RELAXATION = 0.8
CUTOFF = 1.5


MESH = pl.DeviceIdType.MESH


class Segments:
    def __init__(self, count, box, cells):
        self.count, self.box, self.cells = count, box, cells
        self.lines = cells // SIDE // SEGMENTS
        self.across = LANES // (SEGMENTS * count)
        self.deep = box // self.across
        self.length = self.lines * SIDE
        self.tiles = cells // LANES
        self.blocks = -(-self.length // LANES)
        self.shift = count * self.across
        self.stored = (self.deep + 2) * (self.lines + 2)
        assert self.deep * self.across == box and self.length % HALF == 0
        assert self.tiles * LANES == cells and SIDE % 8 == 0 and box % 8 == 0

    def block(self, plane, line):
        return (plane + 1) * (self.lines + 2) + line + 1

    def spread(self, load, store):
        lane = lax.broadcasted_iota(jnp.int32, (self.across, LANES), 1)
        for plane in range(self.deep):
            kept = {}

            def tile_of(orbital, tile, turned):
                if (orbital, tile, turned) not in kept:
                    value = load(orbital, tile, plane)
                    kept[orbital, tile, turned] = pltpu.roll(value, HALF, 1) if turned else value
                return kept[orbital, tile, turned]

            for block in range(self.blocks):
                rows = min(LANES, self.length - block * LANES)
                pieces = []
                for segment in range(SEGMENTS):
                    first = segment * self.length + block * LANES
                    for orbital in range(self.count):
                        parts = []
                        for half in range(2):
                            cell = min(first + half * HALF, self.cells - HALF)
                            turned = cell % LANES != half * HALF
                            parts.append(tile_of(orbital, cell // LANES, turned))
                        if rows <= HALF or parts[0] is parts[1]:
                            pieces.append(parts[0])
                        else:
                            pieces.append(jnp.where(lane < HALF, parts[0], parts[1]))
                turned = jnp.concatenate(pieces, axis=0).T
                for row in range(0, rows, 8):
                    store(plane, block * LANES + row, turned[row : row + 8])

    def gather(self, load, store):
        lane = lax.broadcasted_iota(jnp.int32, (self.across, LANES), 1)
        for plane in range(self.deep):
            sums = {}
            for block in range(self.blocks):
                rows = min(LANES, self.length - block * LANES)
                pieces = [load(plane, block * LANES + row) for row in range(0, rows, 8)]
                if rows < LANES:
                    pieces.append(jnp.zeros((LANES - rows, LANES), jnp.float32))
                turned = jnp.concatenate(pieces, axis=0).T
                for segment in range(SEGMENTS):
                    base = segment * self.shift
                    value = turned[base : base + self.across]
                    for orbital in range(1, self.count):
                        at = base + orbital * self.across
                        value = value + turned[at : at + self.across]
                    sums[segment, block, False] = value

            def half_of(cell, half):
                segment, place = cell // self.length, cell % self.length
                turned = place % LANES != half * HALF
                key = (segment, place // LANES, turned)
                if key not in sums:
                    sums[key] = pltpu.roll(sums[key[0], key[1], False], HALF, 1)
                return sums[key]

            for tile in range(self.tiles):
                low = half_of(tile * LANES, 0)
                high = half_of(tile * LANES + HALF, 1)
                store(plane, tile, low if low is high else jnp.where(lane < HALF, low, high))


def put_cells(shape, target, plane, start, base, value):
    block = slice(shape.block(plane, start), shape.block(plane, start) + value.shape[0])
    target[block, 8 + base : 16 + base, :] = value
    if base == 0:
        target[block, 8 + SIDE : 9 + SIDE, :] = value[:, :1, :]
    if base == SIDE - 8:
        target[block, 7:8, :] = value[:, 7:, :]


def put_faces(shape, target, plane, start, base, value):
    lines, deep, across = shape.lines, shape.deep, shape.across
    count = value.shape[0]
    cells = slice(8 + base, 16 + base)

    def turn(part, amount):
        return pltpu.roll(part.reshape(-1, LANES), amount, 1).reshape(part.shape)

    def at(plane, line, number):
        first = shape.block(plane, line)
        return slice(first, first + number)

    lane = lax.broadcasted_iota(jnp.int32, value.shape, 2) % across
    if plane == deep - 1:
        target[at(-1, start, count), cells, :] = jnp.where(lane != 0, turn(value, 1), 0.0)
    if plane == 0:
        target[at(deep, start, count), cells, :] = jnp.where(
            lane != across - 1, turn(value, LANES - 1), 0.0
        )
    if start == 0:
        target[at(plane, lines, 1), cells, :] = turn(value[:1], LANES - shape.shift)
    if start + count == lines:
        target[at(plane, -1, 1), cells, :] = turn(value[count - 1 :], shape.shift)


def filter_step(shape, source, target, scale, inverse, first):
    lines, deep = shape.lines, shape.deep
    for base in range(0, SIDE, 8):
        cells = slice(8 + base, 16 + base)
        for start in range(0, lines, GROUP):
            grown = [
                source[shape.block(plane, start - 1) : shape.block(plane, start + GROUP + 1), cells, :]
                if 0 <= plane < deep
                else source[shape.block(plane, start) : shape.block(plane, start + GROUP), cells, :]
                for plane in range(-1, deep + 1)
            ]
            middles = [part[1:-1] if 0 < i <= deep else part for i, part in enumerate(grown)]
            for plane in range(deep):
                first_block = shape.block(plane, start)
                block = slice(first_block, first_block + GROUP)
                rows = slice(plane * lines + start, plane * lines + start + GROUP)
                middle = middles[plane + 1]
                near = source[block, 7 + base : 15 + base, :] + source[block, 9 + base : 17 + base, :]
                near = near + (grown[plane + 1][:-2] + grown[plane + 1][2:])
                near = near + (middles[plane] + middles[plane + 2])
                value = scale[rows, base : base + 8, :] * middle - inverse * near
                if first:
                    value = 0.5 * value
                else:
                    value = value - target[block, cells, :]
                put_cells(shape, target, plane, start, base, value)
                put_faces(shape, target, plane, start, base, value)


def cycles_kernel(doms, ranks, *refs):
    (
        orbitals_hbm, occupations, occupied, weights, ionic_hbm, core_hbm, hartree_hbm,
        output,
        planes_of, ionic, core, flat, weight_rows, even, odd, scale, charge,
        weighted, rim_in, parts, near_h, near_d, work, relaxed, grown, local, box_pot, sums, dom_sums,
        load_sem, rim_send, rim_recv, part_send, part_recv, h_send, h_recv, d_send, d_recv,
        sum_send, sum_recv, dom_send, dom_recv, box_send, box_recv, relay_send,
    ) = refs
    count, box, cells = orbitals_hbm.shape
    chunks, planes, _ = weighted.shape
    shape = Segments(count, box, cells)
    tiles = shape.tiles
    rim = BUF // planes
    span = near_h.shape[1]
    reach = span // 2
    assert planes + 2 * (SWEEPS - 2) <= 8
    everyone = doms * ranks
    dom = lax.axis_index("dom")
    rank = lax.axis_index("orb")
    me = dom * ranks + rank

    def place(index):
        return (lax.div(index, ranks), lax.rem(index, ranks))

    def send(source, target, send_sem, recv_sem, to):
        return pltpu.make_async_remote_copy(
            src_ref=source, dst_ref=target, send_sem=send_sem, recv_sem=recv_sem,
            device_id=to, device_id_type=MESH,
        )

    def repeat(low, high, step):
        lax.fori_loop(low, high, lambda i, carry: (step(i), carry)[1], 0)

    def outward(low, high, step):
        def both(i):
            pl.when(ranks - 1 - i > rank)(lambda: step(ranks - 1 - i))
            pl.when(i < rank)(lambda: step(i))

        repeat(low, high, both)

    def arrived(target, sem):
        send(target, target, sem, sem, (dom, rank)).wait_recv()

    def left(source, sem):
        send(source, source, sem, sem, (dom, rank)).wait_send()

    def loads(source, target, sem):
        for tile in range(tiles):
            pltpu.make_async_copy(
                source.at[:, tile * LANES : (tile + 1) * LANES],
                target.at[tile],
                sem,
            ).start()

    def loaded(target, sem):
        pltpu.make_async_copy(target, target, sem).wait()

    loads(ionic_hbm, ionic, load_sem.at[0])
    for orbital in range(count):
        loads(orbitals_hbm.at[orbital], planes_of.at[orbital], load_sem.at[1])
    guess = pltpu.make_async_copy(hartree_hbm, near_h.at[0, reach], load_sem.at[2])
    guess.start()

    barrier = pltpu.get_barrier_semaphore()

    def greet(to):
        pl.semaphore_signal(barrier, inc=1, device_id=to, device_id_type=MESH)

    repeat(1, ranks, lambda k: greet((dom, lax.rem(rank + k, ranks))))
    repeat(1, doms, lambda k: greet((lax.rem(dom + k, doms), rank)))
    for k in range(1, reach + 1):
        greet(place(lax.rem(me + k, everyone)))
        greet(place(lax.rem(me - k + everyone, everyone)))

    lane = lax.broadcasted_iota(jnp.int32, (8, LANES), 1)
    orbital_of = lax.rem(lax.div(lane, shape.across), count)

    def strided(ref, tile, plane):
        return ref[tile, pl.ds(plane, shape.across, stride=shape.deep), :]

    def store_orbitals(plane, cell, value):
        put_cells(shape, even, plane, cell // SIDE, cell % SIDE, value[None])

    def store_scale(plane, cell, value):
        scale[plane * shape.lines + cell // SIDE, cell % SIDE : cell % SIDE + 8, :] = value

    def near_copies(cycle, buffer, send_sems, recv_sems):
        copies = []
        for k in range(1, reach + 1):
            for sign in (1, -1):
                to = place(lax.rem(me + sign * k + everyone, everyone))
                slot = reach - sign * k
                copies.append(
                    send(
                        buffer.at[cycle, reach], buffer.at[cycle, slot],
                        send_sems.at[cycle], recv_sems.at[cycle], to,
                    )
                )
        return copies

    factors = []
    for orbital in range(count):
        taken = rank * count + orbital < occupied[0, 0]
        factors.append(
            jnp.where(taken, occupations[0, orbital], jnp.float32(0.0)) / (ranks * count)
        )
    norms = [jnp.float32(1.0)] * count
    height = work.shape[0]
    origin = reach * planes - 2

    def put(target, slot, value):
        run = min(planes, 2)
        for row in range(0, planes, run):
            at = (slot * planes + row - origin) % height
            target[at : at + run, :] = value[row : row + run]

    def relax(field, added):
        for sweep in range(SWEEPS):
            if field is None:
                field = added
                continue
            near = pltpu.roll(field, 1, 0) + pltpu.roll(field, field.shape[0] - 1, 0)
            if sweep == 1:
                field, near = field[:8], near[:8]
            column = lax.broadcasted_iota(jnp.int32, field.shape, 1) % SIDE
            left = jnp.where(
                column == 0, pltpu.roll(field, cells - (SIDE - 1), 1), pltpu.roll(field, 1, 1)
            )
            right = jnp.where(
                column == SIDE - 1, pltpu.roll(field, SIDE - 1, 1),
                pltpu.roll(field, cells - 1, 1),
            )
            near = near + left + right
            near = near + pltpu.roll(field, SIDE, 1) + pltpu.roll(field, cells - SIDE, 1)
            field = field + RELAXATION * (near * (1.0 / 6.0) - field)
            if added is not None:
                field = field + added[: field.shape[0]]
        return field

    work[...] = jnp.zeros_like(work)
    h_copies = None

    for cycle in range(CYCLES):
        last = cycle + 1 == CYCLES
        if cycle == 0:
            loaded(ionic, load_sem.at[0])
            flat[...] = ionic[...]
        else:
            for tile in range(tiles):
                lanes = slice(tile * LANES, (tile + 1) * LANES)
                for group in range(0, box, 8):
                    first = group // planes
                    pieces = [box_pot[first + i, :, lanes] for i in range(8 // planes)]
                    flat[tile, group : group + 8, :] = ionic[
                        tile, group : group + 8, :
                    ] + jnp.concatenate(pieces, axis=0)
        potential = flat[...]
        lowest = jnp.min(jnp.min(potential, axis=0), axis=0, keepdims=True)
        lowest = jnp.min(lowest, axis=1, keepdims=True)
        highest = jnp.max(jnp.max(potential, axis=0), axis=0, keepdims=True)
        highest = jnp.max(highest, axis=1, keepdims=True)
        low_bound = lowest + CUTOFF
        high_bound = highest + 6.0
        center = 0.5 * (high_bound + low_bound)
        inverse = 1.0 / (0.5 * (high_bound - low_bound))
        flat[...] = (2.0 * inverse) * ((3.0 - center) + potential)
        shape.spread(lambda _, tile, plane: strided(flat, tile, plane), store_scale)
        if cycle == 0:
            loaded(planes_of, load_sem.at[1])
            shape.spread(
                lambda orbital, tile, plane: strided(planes_of.at[orbital], tile, plane),
                store_orbitals,
            )
            for base in range(0, SIDE, 8):
                for start in range(0, shape.lines, GROUP):
                    for plane in range(shape.deep):
                        first = shape.block(plane, start)
                        value = even[first : first + GROUP, 8 + base : 16 + base, :]
                        put_faces(shape, even, plane, start, base, value)

        filter_step(shape, even, odd, scale, inverse, True)
        if cycle == 0:
            pl.semaphore_wait(barrier, ranks + doms - 2 + 2 * reach)
            loads(core_hbm, core, load_sem.at[3])
            guess.wait()
        for copy in near_copies(cycle, near_h, h_send, h_recv):
            copy.start()
        if cycle == 0:
            sublane = lax.broadcasted_iota(jnp.int32, (8, LANES), 0)
            for group in range(0, box, 8):
                rows = jnp.full((8, LANES), weights[0, group], jnp.float32)
                for row in range(1, 8):
                    rows = jnp.where(sublane == row, weights[0, group + row], rows)
                weight_rows[group : group + 8, :] = rows

        def two_steps(step, carry):
            filter_step(shape, odd, even, scale, inverse, False)
            filter_step(shape, even, odd, scale, inverse, False)
            return carry

        lax.fori_loop(0, (DEGREE - 1) // 2, two_steps, 0)
        filter_step(shape, odd, even, scale, inverse, False)

        total = jnp.zeros((8, LANES), jnp.float32)
        for base in range(0, SIDE, 8):
            for plane in range(shape.deep):
                value = even[
                    shape.block(plane, 0) : shape.block(plane, shape.lines), 8 + base : 16 + base, :
                ]
                total = total + jnp.sum(value * value, axis=0)
        shares = jnp.zeros((8, LANES), jnp.float32)
        for orbital in range(count):
            square = jnp.sum(
                jnp.where(orbital_of == orbital, total, 0.0), axis=0, keepdims=True
            )
            square = jnp.sum(square, axis=1, keepdims=True)
            square = norms[orbital] * square * (1.0 / (box * cells)) + 1e-06
            share = factors[orbital] * norms[orbital] / square
            shares = jnp.where(orbital_of == orbital, share, shares)
            norms[orbital] = norms[orbital] / square

        def load_density(plane, cell):
            at = cell % SIDE
            value = even[shape.block(plane, cell // SIDE), 8 + at : 16 + at, :]
            return shares * (value * value)

        def store_density(plane, tile, value):
            flat[tile, pl.ds(plane, shape.across, stride=shape.deep), :] = value

        shape.gather(load_density, store_density)
        if cycle == 0:
            loaded(core, load_sem.at[3])
        def weigh(groups, found):
            for group in groups:
                rows = slice(group, group + 8)
                weight = weight_rows[rows, :]
                for tile in range(tiles):
                    density = flat[tile, rows, :] + core[tile, rows, :] * (1.0 / ranks)
                    density = density * weight
                    found = found + density
                    for piece in range(8 // planes):
                        weighted[
                            group // planes + piece, :, tile * LANES : (tile + 1) * LANES
                        ] = density[piece * planes : (piece + 1) * planes]
            return found

        outer = list(range(0, BUF, 8)) + list(range(box - BUF, box, 8))
        edges = list(range(BUF, 2 * BUF, 8)) + list(range(box - 2 * BUF, box - BUF, 8))
        found = jnp.zeros((8, LANES), jnp.float32) if cycle == 0 else charge[...]
        found = weigh(outer, found)
        down = (lax.rem(dom + doms - 1, doms), rank)
        up = (lax.rem(dom + 1, doms), rank)
        rims = [
            send(
                weighted.at[:rim], rim_in.at[cycle, 1],
                rim_send.at[cycle], rim_recv.at[cycle, 1], down,
            ),
            send(
                weighted.at[rim + ranks :], rim_in.at[cycle, 0],
                rim_send.at[cycle], rim_recv.at[cycle, 0], up,
            ),
        ]
        for copy in rims:
            copy.start()
        found = weigh([g for g in range(2 * BUF, box - 2 * BUF, 8)], found)

        def sum_copy(k):
            to = (dom, lax.rem(rank + k, ranks))
            return send(sums.at[rank], sums.at[rank], sum_send.at[0], sum_recv.at[0], to)

        def part_copy(owner, cycle=cycle):
            return send(
                weighted.at[owner + rim], parts.at[cycle, rank],
                part_send.at[cycle], part_recv.at[cycle], (dom, owner),
            )

        def give(owner):
            part_copy(owner).start()

        def delayed(owner):
            apart = (2 * owner >= ranks) != (2 * rank >= ranks)
            return jnp.logical_and(apart, lax.rem(owner + rank, 2) == 0)

        def give_now(owner):
            pl.when(jnp.logical_not(delayed(owner)))(lambda: give(owner))

        def give_later(owner):
            pl.when(delayed(owner))(lambda: give(owner))

        outward(rim, ranks - rim, give_now)
        found = weigh(edges, found)
        if last:
            sums[rank] = found
            repeat(1, ranks, lambda k: sum_copy(k).start())
        else:
            charge[...] = found

        def join(step):
            side = lax.rem(dom + 1 + step, 2)
            arrived(rim_in.at[cycle, side], rim_recv.at[cycle, side])
            base = side * (ranks - rim)
            for j in range(rim):
                weighted[rim + base + j] += rim_in[cycle, side, j]
                pl.when(base + j != rank)(lambda: give(base + j))

        repeat(0, 2, join)
        outward(rim, ranks - rim, give_later)

        arrived(near_h.at[cycle, : span - 1], h_recv.at[cycle])
        for slot in range(span):
            put(work, slot, near_h[cycle, slot])
        relaxed[...] = relax(work[...], None)

        def dom_copy(k):
            to = (lax.rem(dom + k, doms), rank)
            return send(dom_sums.at[dom], dom_sums.at[dom], dom_send.at[0], dom_recv.at[0], to)

        arrived(parts.at[cycle, : ranks - 1], part_recv.at[cycle])
        density = weighted[rank + rim]
        for k in range(1, ranks):
            density = density + parts[cycle, lax.rem(rank + k, ranks)]
        near_d[cycle, reach] = density
        d_copies = near_copies(cycle, near_d, d_send, d_recv)
        for copy in d_copies:
            copy.start()

        if last:
            arrived(sums.at[: ranks - 1], sum_recv.at[0])
            dom_sums[dom] = jnp.sum(sums[...], axis=0)
            repeat(1, doms, lambda k: dom_copy(k).start())

        root = jnp.exp(jnp.log(density) * (1.0 / 3.0))
        root = root - (root - density / (root * root)) * (1.0 / 3.0)
        local[...] = relaxed[2 : 2 + planes, :] - EXCHANGE_FACTOR * root
        arrived(near_d.at[cycle, : span - 1], d_recv.at[cycle])
        for slot in range(span):
            put(work, slot, near_d[cycle, slot])
        if last:
            arrived(dom_sums.at[: doms - 1], dom_recv.at[0])
            total = jnp.sum(jnp.sum(dom_sums[...], axis=0), axis=0, keepdims=True)
            total = jnp.sum(total, axis=1, keepdims=True)
            average = total / (everyone * planes * cells)
            shift = (-SWEEPS * RELAXATION * FOUR_PI / 6.0) * average
            local[...] += shift
        change = relax(None, (RELAXATION * FOUR_PI / 6.0) * work[...])
        grown[...] = change
        change = grown[2 : 2 + planes, :]
        result = local[...] + change

        left(near_h.at[cycle, : span - 1], h_send.at[cycle])
        if not last:
            slot = rank + rim
            box_pot[slot] = result

            late = jnp.where(rank >= ranks - rim, rank - (ranks - 2 * rim), 2 * rim)
            box_sem = jnp.where(rank < rim, rank, late)

            def box_copy(to):
                return send(
                    box_pot.at[rank + rim], box_pot.at[rank + rim],
                    box_send.at[0], box_recv.at[box_sem], (dom, to),
                )

            outward(0, ranks, lambda to: box_copy(to).start())
            near_h[cycle + 1, reach] = relaxed[2 : 2 + planes, :] + change

            def relay_copy(index):
                side, j = lax.div(index, rim), lax.rem(index, rim)
                owner = side * (ranks - rim) + j
                target = jnp.where(side == 0, chunks - rim + j, j)
                to_dom = lax.rem(dom + jnp.where(side == 0, doms - 1, 1), doms)
                return send(
                    box_pot.at[owner + rim], box_pot.at[target],
                    relay_send.at[0], box_recv.at[2 * rim], (to_dom, rank),
                )

            def relay(step):
                index = lax.rem(step + rim * lax.rem(dom + 1, 2), 2 * rim)
                side, j = lax.div(index, rim), lax.rem(index, rim)
                owner = side * (ranks - rim) + j

                @pl.when(owner != rank)
                def _():
                    arrived(box_pot.at[owner + rim], box_recv.at[index])

                relay_copy(index).start()

            repeat(0, 2 * rim, relay)
            at_edge = box_sem < 2 * rim

            @pl.when(at_edge)
            def _():
                arrived(box_pot.at[:ranks], box_recv.at[2 * rim])

            @pl.when(jnp.logical_not(at_edge))
            def _():
                arrived(box_pot.at[: ranks - 1], box_recv.at[2 * rim])

            left(box_pot.at[: ranks - 1], box_send.at[0])
            left(box_pot.at[: 2 * rim], relay_send.at[0])

        left(rim_in.at[cycle], rim_send.at[cycle])
        left(near_d.at[cycle, : span - 1], d_send.at[cycle])
        left(parts.at[cycle, : ranks - 1], part_send.at[cycle])
        if last:
            output[...] = result
            left(sums.at[: ranks - 1], sum_send.at[0])
            left(dom_sums.at[: doms - 1], dom_send.at[0])


def body(
    orbitals, occupations, occupied_count, weights, external_potential, core_density, hartree_guess
):
    doms, ranks = lax.axis_size("dom"), lax.axis_size("orb")
    count, box, cells = orbitals.shape[1:]
    planes = hartree_guess.shape[0]
    chunks = box // planes
    rim = BUF // planes
    reach = -(-SWEEPS // planes)
    span = 2 * reach + 1
    rows = -(-span * planes // 8) * 8
    shape = Segments(count, box, cells)
    lines = shape.deep * shape.lines
    f32 = jnp.float32
    anywhere = pl.BlockSpec(memory_space=pl.ANY)
    scalars = pl.BlockSpec(memory_space=pltpu.SMEM)
    dma = pltpu.SemaphoreType.DMA
    vmem = lambda *dims: pltpu.VMEM(dims, f32)
    return pl.pallas_call(
        functools.partial(cycles_kernel, doms, ranks),
        out_shape=pltpu.VMEM((planes, cells), f32),
        in_specs=[anywhere, scalars, scalars, scalars, anywhere, anywhere, anywhere],
        out_specs=pl.BlockSpec(memory_space=pltpu.VMEM),
        scratch_shapes=[
            vmem(count, shape.tiles, box, LANES),
            vmem(shape.tiles, box, LANES),
            vmem(shape.tiles, box, LANES),
            vmem(shape.tiles, box, LANES),
            vmem(box, LANES),
            vmem(shape.stored, PITCH, LANES),
            vmem(shape.stored, PITCH, LANES),
            vmem(lines, SCALE_PITCH, LANES),
            vmem(8, LANES),
            vmem(chunks, planes, cells),
            vmem(CYCLES, 2, rim, planes, cells),
            vmem(CYCLES, ranks, planes, cells),
            vmem(CYCLES, span, planes, cells),
            vmem(CYCLES, span, planes, cells),
            vmem(rows, cells),
            vmem(8, cells),
            vmem(8, cells),
            vmem(planes, cells),
            vmem(chunks, planes, cells),
            vmem(ranks, 8, LANES),
            vmem(doms, 8, LANES),
            dma((4,)),
            dma((CYCLES,)), dma((CYCLES, 2)),
            dma((CYCLES,)), dma((CYCLES,)),
            dma((CYCLES,)), dma((CYCLES,)),
            dma((CYCLES,)), dma((CYCLES,)),
            dma((1,)), dma((1,)),
            dma((1,)), dma((1,)),
            dma((1,)), dma((2 * rim + 1,)),
            dma((1,)),
        ],
        compiler_params=pltpu.CompilerParams(collective_id=0, has_side_effects=True),
        name="cycles",
    )(
        orbitals[0], occupations, occupied_count.reshape(1, 1), weights, external_potential[0],
        core_density[0], hartree_guess,
    )


def solution(mesh):
    placed = (
        P("dom", "orb", None, None),
        P("dom", "orb"),
        P("dom"),
        P("dom", None),
        P("dom", None, None),
        P("dom", None, None),
        P(("dom", "orb"), None),
    )
    return jax.shard_map(
        body, mesh=mesh, in_specs=placed, out_specs=P(("dom", "orb"), None), check_vma=False
    )
```
